8 devices in a mesh: dp: 2 (over z, y), row: 2 (over x), fsdp: 2 (over core).
Axes of the slice: x: 2, y: 2, z: 1, core: 2. Of those that a mesh axis runs over, the one named last changes fastest.
Arguments:
- x_saved: bfloat16 [2, 24576, 768], P(None, ('dp', 'row', 'fsdp'))
- dy_out: bfloat16 [2, 24576, 768], P(None, ('dp', 'row', 'fsdp'))
- w_gate: bfloat16 [768, 2048], P(None, ('row', 'fsdp'))
- w_up: bfloat16 [768, 2048], P(None, ('row', 'fsdp'))
- w_down: bfloat16 [2048, 768], P(('row', 'fsdp'))
- g_next: float32 [8, 3, 768, 2048], P(('dp', 'row', 'fsdp'))
Outputs:
- output 1: bfloat16 [2, 24576, 768], P(None, ('dp', 'row', 'fsdp'))
- output 2: float32 [3, 768, 2048], P(None, None, ('row', 'fsdp'))
- output 3: float32 [8, 3, 768, 2048], P(('dp', 'row', 'fsdp'))
All inputs are finite; a program needn't handle non-finite values.
Results may differ from the reference program's by a relative error of at most 0.00911145.
Values are sent between devices in bfloat16 or wider.
A program may use at most 1 GiB of HBM per device.

```python
import jax
import jax.numpy as jnp
from jax import lax

DEVICES = 8
TOK_DEV = 3072
D_MODEL = 768
FF_DIM = 2048
MICRO_COUNT = 2


def setup_inputs(seed: int = 0) -> dict:
    key_list = jax.random.split(jax.random.key(seed), 6)
    tok_all = DEVICES * TOK_DEV
    act_shape = (MICRO_COUNT, tok_all, D_MODEL)
    x_saved = jax.random.normal(key_list[0], act_shape, jnp.float32)
    dy_out = jax.random.normal(key_list[1], act_shape, jnp.float32)
    w_gate = jax.random.normal(key_list[2], (D_MODEL, FF_DIM), jnp.float32) * D_MODEL ** -0.5
    w_up = jax.random.normal(key_list[3], (D_MODEL, FF_DIM), jnp.float32) * D_MODEL ** -0.5
    w_down = jax.random.normal(key_list[4], (FF_DIM, D_MODEL), jnp.float32) * FF_DIM ** -0.5
    g_next = jax.random.normal(key_list[5], (DEVICES, 3, D_MODEL, FF_DIM), jnp.float32) * DEVICES ** -0.5
    return {"x_saved": x_saved.astype(jnp.bfloat16), "dy_out": dy_out.astype(jnp.bfloat16), "w_gate": w_gate.astype(jnp.bfloat16), "w_up": w_up.astype(jnp.bfloat16), "w_down": w_down.astype(jnp.bfloat16), "g_next": g_next}


def silu_slope(pre_act):
    sigmoid_val = jax.nn.sigmoid(pre_act)
    return sigmoid_val * (1.0 + pre_act * (1.0 - sigmoid_val))


def device_backward(x_dev, dy_dev, w_gate, w_up, w_down):
    def one_micro(grad_acc, micro_pair):
        x_mb, dy_mb = micro_pair
        pre_gate = jnp.dot(x_mb, w_gate, preferred_element_type=jnp.float32)
        pre_up = jnp.dot(x_mb, w_up, preferred_element_type=jnp.float32)
        act_gate = jax.nn.silu(pre_gate)
        hidden = (act_gate * pre_up).astype(jnp.bfloat16)
        d_hidden = jnp.dot(dy_mb, w_down.T, preferred_element_type=jnp.float32)
        d_gate = (d_hidden * pre_up * silu_slope(pre_gate)).astype(jnp.bfloat16)
        d_up = (d_hidden * act_gate).astype(jnp.bfloat16)
        dx_mb = (jnp.dot(d_gate, w_gate.T, preferred_element_type=jnp.float32) + jnp.dot(d_up, w_up.T, preferred_element_type=jnp.float32)).astype(jnp.bfloat16)
        grad_mb = jnp.stack([
            jnp.dot(x_mb.T, d_gate, preferred_element_type=jnp.float32),
            jnp.dot(x_mb.T, d_up, preferred_element_type=jnp.float32),
            jnp.dot(dy_mb.T, hidden, preferred_element_type=jnp.float32),
        ])
        return grad_acc + grad_mb, dx_mb

    grad_init = jnp.zeros((3, D_MODEL, FF_DIM), jnp.float32)
    grad_sum, dx_dev = lax.scan(one_micro, grad_init, (x_dev, dy_dev))
    return dx_dev, grad_sum


def reference(x_saved, dy_out, w_gate, w_up, w_down, g_next):
    x_dev = x_saved.reshape(MICRO_COUNT, DEVICES, TOK_DEV, D_MODEL).transpose(1, 0, 2, 3)
    dy_dev = dy_out.reshape(MICRO_COUNT, DEVICES, TOK_DEV, D_MODEL).transpose(1, 0, 2, 3)

    def per_device(dev_pair):
        return device_backward(dev_pair[0], dev_pair[1], w_gate, w_up, w_down)

    dx_dev, grad_layer = lax.map(per_device, (x_dev, dy_dev))
    dx_out = dx_dev.transpose(1, 0, 2, 3).reshape(MICRO_COUNT, DEVICES * TOK_DEV, D_MODEL)
    grad_next = jnp.sum(g_next.astype(jnp.bfloat16).astype(jnp.float32), axis=0)
    return dx_out, grad_next, grad_layer
```

```python
import functools

import jax
import jax.numpy as jnp
from jax import lax
from jax.experimental import pallas as pl
from jax.experimental.pallas import tpu as pltpu
from jax.sharding import PartitionSpec as P

TOK_AXES = ("dp", "row", "fsdp")
GROUP_AXES = ("row", "fsdp")
TILE = 1024
VMEM_BYTES = 64 * 1024 * 1024
SWAP = [(0, 1), (1, 0)]


def dot(lhs, rhs, lhs_dim, rhs_dim):
    return lax.dot_general(lhs, rhs, (((lhs_dim,), (rhs_dim,)), ((), ())), preferred_element_type=jnp.float32)


def backward_tile(x_ref, dy_ref, w13_ref, w2_ref, z_ref, h_ref, dw_ref, first):
    ff = h_ref.shape[1]
    ab = dot(x_ref[...], w13_ref[...], 1, 0)
    dh = dot(dy_ref[...], w2_ref[...], 1, 1)
    gate, up = ab[:, :ff], ab[:, ff:]
    sig = jax.nn.sigmoid(gate)
    act = gate * sig
    h_ref[...] = (act * up).astype(jnp.bfloat16)
    z_ref[:, :ff] = (dh * up * (sig + act * (1.0 - sig))).astype(jnp.bfloat16)
    z_ref[:, ff:] = (dh * act).astype(jnp.bfloat16)
    dx = dot(z_ref[...], w13_ref[...], 1, 1)

    @pl.when(first)
    def _():
        dw_ref[...] = jnp.zeros_like(dw_ref)

    dw13 = dot(x_ref[...], z_ref[...], 0, 0)
    dw_ref[0] += dw13[:, :ff]
    dw_ref[1] += dw13[:, ff:]
    dw_ref[2] += dot(dy_ref[...], h_ref[...], 0, 0)
    return dx


def shards_kernel(last, cols_ref, x_ref, dy_ref, *refs):
    w_refs, refs = refs[:6], refs[6:]
    dxp_ref = None
    if last:
        dxp_ref, _, *refs = refs
    dx_ref, dw_ref, acc_ref, w13_ref, w2_ref, z_ref, h_ref = refs
    shard, tile = pl.program_id(0), pl.program_id(1)
    ff = h_ref.shape[1]
    for s in range(2):
        @pl.when((shard == s) & (tile == 0))
        def _():
            w13_ref[:, :ff] = w_refs[3 * s][...]
            w13_ref[:, ff:] = w_refs[3 * s + 1][...]
            w2_ref[...] = w_refs[3 * s + 2][...]

    dx = backward_tile(x_ref, dy_ref, w13_ref, w2_ref, z_ref, h_ref, dw_ref, tile == 0)
    rows = pl.ds(pl.multiple_of(tile * TILE, TILE), TILE)

    @pl.when(shard == 0)
    def _():
        acc_ref[rows, :] = dx + dxp_ref[...] if last else dx

    @pl.when(shard == 1)
    def _():
        dx_ref[...] = (acc_ref[rows, :] + dx).astype(dx_ref.dtype)


def two_shards(cols, x, dy, weights, partial=None):
    tokens, d = x.shape
    ff = weights[0].shape[1]
    tiles = tokens // TILE
    last = partial is not None
    tok = pl.BlockSpec((TILE, d), lambda s, j, c: (j, 0))
    full = lambda w: pl.BlockSpec(w.shape, lambda s, j, c: (0, 0))
    in_specs = [tok, tok] + [full(w) for w in weights]
    args = [cols, x, dy, *weights]
    if last:
        in_specs += [pl.BlockSpec((TILE, d), lambda s, j, c: (jnp.where(s == 0, j, tiles - 1), 0)), pl.BlockSpec(memory_space=pl.ANY)]
        args += partial
    flops = 2 * 8 * 2 * tokens * d * ff
    return pl.pallas_call(
        functools.partial(shards_kernel, last),
        grid_spec=pltpu.PrefetchScalarGridSpec(
            num_scalar_prefetch=1,
            grid=(2, tiles),
            in_specs=in_specs,
            out_specs=[
                pl.BlockSpec((TILE, d), lambda s, j, c: (jnp.where(s == 1, j, 0), 0)),
                pl.BlockSpec((3, d, ff), lambda s, j, c: (0, 0, c[s])),
            ],
            scratch_shapes=[
                pltpu.VMEM((tokens, d), jnp.float32),
                pltpu.VMEM((d, 2 * ff), jnp.bfloat16),
                pltpu.VMEM((ff, d), jnp.bfloat16),
                pltpu.VMEM((TILE, 2 * ff), jnp.bfloat16),
                pltpu.VMEM((TILE, ff), jnp.bfloat16),
            ],
        ),
        out_shape=[
            jax.ShapeDtypeStruct((tokens, d), jnp.bfloat16 if last else jnp.float32),
            jax.ShapeDtypeStruct((3, d, 4 * ff), jnp.float32),
        ],
        input_output_aliases={len(args) - 1: 1} if last else {},
        compiler_params=pltpu.CompilerParams(vmem_limit_bytes=VMEM_BYTES, dimension_semantics=("arbitrary", "arbitrary")),
        cost_estimate=pl.CostEstimate(flops=flops, bytes_accessed=100_000_000, transcendentals=0),
        name="bwd_last" if last else "bwd_first",
    )(*args)


def solution(mesh):
    def local_step(x_dev, dy_dev, gate_shard, up_shard, down_shard, g_dev):
        row, core = lax.axis_index("row"), lax.axis_index("fsdp")
        own = [gate_shard, up_shard, down_shard]
        mate = [lax.ppermute(w, "fsdp", SWAP) for w in own]
        far = [lax.ppermute(w, "row", SWAP) for w in own]

        g_shard = lax.psum_scatter(g_dev[0].astype(jnp.bfloat16), GROUP_AXES, scatter_dimension=2, tiled=True)
        g_other = lax.ppermute(g_shard, "dp", SWAP)
        grad_next = g_shard.astype(jnp.float32) + g_other.astype(jnp.float32)

        micro_count, tok_dev, d_model = x_dev.shape
        x, dy = (v.reshape(micro_count * tok_dev, d_model) for v in (x_dev, dy_dev))
        cols = lambda r: jnp.stack([2 * r + core, 2 * r + 1 - core]).astype(jnp.int32)
        partial = two_shards(cols(row), x, dy, own + mate)
        far, partial = lax.optimization_barrier((far, partial))
        far_mate = [lax.ppermute(w, "fsdp", SWAP) for w in far]
        dx, grad_layer = two_shards(cols(1 - row), x, dy, far + far_mate, partial)
        return dx.reshape(micro_count, tok_dev, d_model), grad_next, grad_layer[None]

    in_specs = (P(None, TOK_AXES, None), P(None, TOK_AXES, None), P(None, GROUP_AXES), P(None, GROUP_AXES), P(GROUP_AXES, None), P(TOK_AXES, None, None, None))
    out_specs = (P(None, TOK_AXES, None), P(None, None, GROUP_AXES), P(TOK_AXES, None, None, None))
    return jax.shard_map(local_step, mesh=mesh, in_specs=in_specs, out_specs=out_specs, check_vma=False)
```

```python
import functools

import jax
import jax.numpy as jnp
from jax import lax
from jax.experimental import pallas as pl
from jax.experimental.pallas import tpu as pltpu
from jax.sharding import PartitionSpec as P

TOK_AXES = ("dp", "row", "fsdp")
GROUP_AXES = ("row", "fsdp")
VMEM_BYTES = 67_000_000
MESH = pl.DeviceIdType.MESH

TILE1 = 768
TILE2 = 1024
SHARDS1 = 3
CHUNKS = 16
CORE_SUM = 3
ROW_SUM = 13
FORWARD = 12


def dot(lhs, rhs, lhs_dim, rhs_dim):
    return lax.dot_general(lhs, rhs, (((lhs_dim,), (rhs_dim,)), ((), ())), preferred_element_type=jnp.float32)


def wide_sum(a, b):
    return (a.astype(jnp.float32) + b.astype(jnp.float32)).astype(jnp.bfloat16)


def backward_tile(x_ref, dy_ref, w13, w2, z_ref, h_ref, dw_ref, first, rows, put_dx):
    tile, ff = h_ref.shape
    for r in range(tile // rows):
        sl = slice(r * rows, (r + 1) * rows)
        ab = dot(x_ref[sl, :], w13[...], 1, 0)
        dh = dot(dy_ref[sl, :], w2[...], 1, 1)
        gate, up = ab[:, :ff], ab[:, ff:]
        sig = jax.nn.sigmoid(gate)
        act = gate * sig
        h_ref[sl, :] = (act * up).astype(jnp.bfloat16)
        z_ref[sl, :ff] = (dh * up * (sig + act * (1.0 - sig))).astype(jnp.bfloat16)
        z_ref[sl, ff:] = (dh * act).astype(jnp.bfloat16)
        put_dx(r, dot(z_ref[sl, :], w13[...], 1, 1))
    dw13 = dot(x_ref[...], z_ref[...], 0, 0)
    terms = (dw13[:, :ff], dw13[:, ff:], dot(dy_ref[...], h_ref[...], 0, 0))
    for slab, term in enumerate(terms):
        dw_ref[slab] = jnp.where(first, 0.0, dw_ref[slab]) + term


def first_kernel(
    x_ref, dy_ref, g_ref, w1_ref, w3_ref, w2_ref,
    dxp_ref, dws_ref, f1_ref, f3_ref, f2_ref, r_ref, c_ref,
    acc_ref, w13s_ref, w2s_ref, z_ref, h_ref, send_ref, own_ref, core_ref, row_ref,
    w_loc, w_core, w_row, w_fwd, a_sem, b_sem, c_sem, out_sem, dx_sem,
):
    shard, tile = pl.program_id(0), pl.program_id(1)
    tiles = pl.num_programs(1)
    step = shard * tiles + tile
    steps = SHARDS1 * tiles
    dp, row, core = (lax.axis_index(a) for a in TOK_AXES)
    mate = (dp, row, 1 - core)
    across = (dp, 1 - row, core)
    replica = (1 - dp, row, core)
    ff = h_ref.shape[1]
    chunk = g_ref.shape[0]

    def push(src, dst, sems, k, to):
        return pltpu.make_async_remote_copy(
            src_ref=src, dst_ref=dst, send_sem=sems.at[0, k], recv_sem=sems.at[1, k], device_id=to, device_id_type=MESH
        )

    def slots(s):
        return w13s_ref.at[s, :, :ff], w13s_ref.at[s, :, ff:], w2s_ref.at[s]

    weights = (w1_ref, w3_ref, w2_ref)
    local = [pltpu.make_async_copy(w, d, w_loc.at[k]) for k, (w, d) in enumerate(zip(weights, slots(0)))]
    to_mate = [push(w, d, w_core, k, mate) for k, (w, d) in enumerate(zip(weights, slots(1)))]
    to_row = [push(w, d, w_row, k, across) for k, (w, d) in enumerate(zip(weights, slots(2)))]
    forward = [push(w, d, w_fwd, k, mate) for k, (w, d) in enumerate(zip(slots(2), (f1_ref, f3_ref, f2_ref)))]

    def rows_of(c):
        return pl.ds(pl.multiple_of(c * chunk, 16), chunk)

    def core_push(c):
        return push(send_ref.at[lax.rem(c, 2)], core_ref.at[:, rows_of(c), :], a_sem, c, mate)

    def row_push(c):
        return push(own_ref.at[1, rows_of(c), :], row_ref.at[rows_of(c), :], b_sem, c, across)

    def dp_push(c):
        return push(own_ref.at[0, rows_of(c), :], c_ref.at[rows_of(c), :], c_sem, c, replica)

    keep_sum = pltpu.make_async_copy(own_ref.at[0], r_ref, out_sem)

    def dx_rows(t):
        return pl.ds(pl.multiple_of(t * TILE1, TILE1), TILE1)

    def dx_out(t):
        return pltpu.make_async_copy(acc_ref.at[dx_rows(t), :], dxp_ref.at[dx_rows(t), :], dx_sem.at[t])

    @pl.when(step == 0)
    def _():
        barrier = pltpu.get_barrier_semaphore()
        for to in (mate, across, replica):
            pl.semaphore_signal(barrier, inc=1, device_id=to, device_id_type=MESH)
        for copy in local:
            copy.start()
        pl.semaphore_wait(barrier, 3)
        for copy in (*to_row, *to_mate):
            copy.start()
        for copy in local:
            copy.wait()

    @pl.when(step == tiles)
    def _():
        for copy in to_mate:
            copy.wait_recv()

    @pl.when(step == FORWARD)
    def _():
        for copy in to_row:
            copy.wait_recv()
        for copy in forward:
            copy.start()

    @pl.when((step >= 1) & (step <= CHUNKS))
    def _():
        core_push(step - 1).start()

    @pl.when(step < CHUNKS)
    def _():
        @pl.when(step >= 2)
        def _():
            core_push(step - 2).wait_send()

        for k, r in enumerate((row, 1 - row)):
            mine = pl.ds(pl.multiple_of((2 * r + core) * ff, ff), ff)
            theirs = pl.ds(pl.multiple_of((2 * r + 1 - core) * ff, ff), ff)
            own_ref[k, rows_of(step), :] = g_ref[:, mine].astype(jnp.bfloat16)
            send_ref[lax.rem(step, 2), k] = g_ref[:, theirs].astype(jnp.bfloat16)

    @pl.when((step > CORE_SUM) & (step <= CORE_SUM + CHUNKS))
    def _():
        row_push(step - CORE_SUM - 1).start()

    @pl.when((step >= CORE_SUM) & (step < CORE_SUM + CHUNKS))
    def _():
        c = step - CORE_SUM
        core_push(c).wait_recv()
        for k in range(2):
            own_ref[k, rows_of(c), :] = wide_sum(own_ref[k, rows_of(c), :], core_ref[k, rows_of(c), :])

    @pl.when((step > ROW_SUM) & (step <= ROW_SUM + CHUNKS // 2))
    def _():
        for k in range(2):
            dp_push(2 * (step - ROW_SUM - 1) + k).start()

    @pl.when((step >= ROW_SUM) & (step < ROW_SUM + CHUNKS // 2))
    def _():
        for k in range(2):
            c = 2 * (step - ROW_SUM) + k
            row_push(c).wait_recv()
            own_ref[0, rows_of(c), :] = wide_sum(own_ref[0, rows_of(c), :], row_ref[rows_of(c), :])

    @pl.when(step == ROW_SUM + CHUNKS // 2 + 1)
    def _():
        keep_sum.start()

    @pl.when(step > steps - tiles)
    def _():
        dx_out(tile - 1).start()

    rows = TILE1 // 2

    def put_dx(r, dx):
        sl = pl.ds(pl.multiple_of(tile * TILE1 + r * rows, rows), rows)
        acc_ref[sl, :] = jnp.where(shard == 0, 0.0, acc_ref[sl, :]) + dx

    backward_tile(x_ref, dy_ref, w13s_ref.at[shard], w2s_ref.at[shard], z_ref, h_ref, dws_ref.at[0], tile == 0, rows, put_dx)

    @pl.when(step == steps - 1)
    def _():
        dx_out(tile).start()
        for copy in (*to_mate, *to_row):
            copy.wait_send()
        for copy in forward:
            copy.wait()
        core_push(CHUNKS - 2).wait_send()
        core_push(CHUNKS - 1).wait_send()
        for c in range(CHUNKS):
            row_push(c).wait_send()
            dp_push(c).wait()
        keep_sum.wait()
        for t in range(dxp_ref.shape[0] // TILE1):
            dx_out(t).wait()


def run_first(x, dy, weights, g):
    tokens, d = x.shape
    ff = weights[0].shape[1]
    g_rows, g_cols = g.shape
    chunk = g_rows // CHUNKS
    tiles = tokens // TILE1
    hbm = pl.BlockSpec(memory_space=pltpu.HBM)
    tok = pl.BlockSpec((TILE1, d), lambda s, j: (j, 0))
    bf16, f32, dma = jnp.bfloat16, jnp.float32, pltpu.SemaphoreType.DMA
    like = lambda v: jax.ShapeDtypeStruct(v.shape, v.dtype)
    return pl.pallas_call(
        first_kernel,
        grid=(SHARDS1, tiles),
        in_specs=[tok, tok, pl.BlockSpec((chunk, g_cols), lambda s, j: (jnp.minimum(s * tiles + j, CHUNKS - 1), 0)), hbm, hbm, hbm],
        out_specs=[hbm, pl.BlockSpec((1, 3, d, ff), lambda s, j: (s, 0, 0, 0)), hbm, hbm, hbm, hbm, hbm],
        out_shape=[
            jax.ShapeDtypeStruct((tokens, d), f32),
            jax.ShapeDtypeStruct((SHARDS1, 3, d, ff), f32),
            *[like(w) for w in weights],
            jax.ShapeDtypeStruct((g_rows, ff), bf16),
            jax.ShapeDtypeStruct((g_rows, ff), bf16),
        ],
        scratch_shapes=[
            pltpu.VMEM((tokens, d), f32),
            pltpu.VMEM((SHARDS1, d, 2 * ff), bf16),
            pltpu.VMEM((SHARDS1, ff, d), bf16),
            pltpu.VMEM((TILE1, 2 * ff), bf16),
            pltpu.VMEM((TILE1, ff), bf16),
            pltpu.VMEM((2, 2, chunk, ff), bf16),
            pltpu.VMEM((2, g_rows, ff), bf16),
            pltpu.VMEM((2, g_rows, ff), bf16),
            pltpu.VMEM((g_rows, ff), bf16),
            dma((3,)),
            dma((2, 3)),
            dma((2, 3)),
            dma((2, 3)),
            dma((2, CHUNKS)),
            dma((2, CHUNKS)),
            dma((2, CHUNKS)),
            dma(()),
            dma((tiles,)),
        ],
        compiler_params=pltpu.CompilerParams(
            vmem_limit_bytes=VMEM_BYTES, dimension_semantics=("arbitrary", "arbitrary"), collective_id=0, has_side_effects=True
        ),
        cost_estimate=pl.CostEstimate(flops=16 * SHARDS1 * tokens * d * ff, bytes_accessed=120_000_000, transcendentals=0),
        name="bwd_first",
    )(x, dy, g, *weights)


def last_kernel(
    x_ref, dy_ref, dxp_ref, dws_ref, w1_ref, w3_ref, w2_ref, r_ref, c_ref,
    dx_ref, next_ref, dw_ref,
    w13s_ref, z_ref, h_ref, dw_acc, move_sem, own_sem,
):
    tile, tiles = pl.program_id(0), pl.num_programs(0)
    row, core = lax.axis_index("row"), lax.axis_index("fsdp")
    ff = h_ref.shape[1]
    block = dws_ref.shape[2]
    cols = [2 * row + core, 2 * row + 1 - core, 2 * (1 - row) + core, 2 * (1 - row) + 1 - core]
    lanes = [pl.ds(pl.multiple_of(q * ff, ff), ff) for q in cols]
    span = pl.ds(pl.multiple_of(tile * block, block), block)
    moves = [pltpu.make_async_copy(dws_ref.at[s], dw_ref.at[:, span, lanes[s]], move_sem.at[s]) for s in range(SHARDS1)]
    for move in moves:
        move.start()

    @pl.when(tile == 0)
    def _():
        w13s_ref[:, :ff] = w1_ref[...]
        w13s_ref[:, ff:] = w3_ref[...]

    next_ref[...] = r_ref[...].astype(jnp.float32) + c_ref[...].astype(jnp.float32)
    rows = TILE2 // 2

    def put_dx(r, dx):
        sl = slice(r * rows, (r + 1) * rows)
        dx_ref[sl, :] = (dxp_ref[sl, :] + dx).astype(jnp.bfloat16)

    backward_tile(x_ref, dy_ref, w13s_ref, w2_ref, z_ref, h_ref, dw_acc, tile == 0, rows, put_dx)
    for move in moves:
        move.wait()

    @pl.when(tile == tiles - 1)
    def _():
        own = pltpu.make_async_copy(dw_acc, dw_ref.at[:, :, lanes[3]], own_sem)
        own.start()
        own.wait()


def run_last(x, dy, dxp, dws, weights, mine, other):
    tokens, d = x.shape
    ff = weights[0].shape[1]
    tiles = tokens // TILE2
    g_rows = mine.shape[0]
    tok = pl.BlockSpec((TILE2, d), lambda j: (j, 0))
    full = lambda w: pl.BlockSpec(w.shape, lambda j: (0, 0))
    part = pl.BlockSpec((g_rows // tiles, ff), lambda j: (j, 0))
    return pl.pallas_call(
        last_kernel,
        grid=(tiles,),
        in_specs=[tok, tok, tok, pl.BlockSpec((SHARDS1, 3, d // tiles, ff), lambda j: (0, 0, j, 0)), *[full(w) for w in weights], part, part],
        out_specs=[tok, part, pl.BlockSpec(memory_space=pltpu.HBM)],
        out_shape=[
            jax.ShapeDtypeStruct((tokens, d), jnp.bfloat16),
            jax.ShapeDtypeStruct((g_rows, ff), jnp.float32),
            jax.ShapeDtypeStruct((3, d, 4 * ff), jnp.float32),
        ],
        scratch_shapes=[
            pltpu.VMEM((d, 2 * ff), jnp.bfloat16),
            pltpu.VMEM((TILE2, 2 * ff), jnp.bfloat16),
            pltpu.VMEM((TILE2, ff), jnp.bfloat16),
            pltpu.VMEM((3, d, ff), jnp.float32),
            pltpu.SemaphoreType.DMA((SHARDS1,)),
            pltpu.SemaphoreType.DMA(()),
        ],
        compiler_params=pltpu.CompilerParams(vmem_limit_bytes=VMEM_BYTES, dimension_semantics=("arbitrary",)),
        cost_estimate=pl.CostEstimate(flops=16 * tokens * d * ff, bytes_accessed=90_000_000, transcendentals=0),
        name="bwd_last",
    )(x, dy, dxp, dws, *weights, mine, other)


def solution(mesh):
    def local_step(x_dev, dy_dev, gate_shard, up_shard, down_shard, g_dev):
        micro_count, tok_dev, d_model = x_dev.shape
        ff = gate_shard.shape[1]
        x, dy = (v.reshape(micro_count * tok_dev, d_model) for v in (x_dev, dy_dev))
        g = g_dev.reshape(3 * d_model, 4 * ff)
        dxp, dws, *far, mine, other = run_first(x, dy, (gate_shard, up_shard, down_shard), g)
        dx, grad_next, grad_layer = run_last(x, dy, dxp, dws, far, mine, other)
        return dx.reshape(micro_count, tok_dev, d_model), grad_next.reshape(3, d_model, ff), grad_layer[None]

    in_specs = (P(None, TOK_AXES, None), P(None, TOK_AXES, None), P(None, GROUP_AXES), P(None, GROUP_AXES), P(GROUP_AXES, None), P(TOK_AXES, None, None, None))
    out_specs = (P(None, TOK_AXES, None), P(None, None, GROUP_AXES), P(TOK_AXES, None, None, None))
    return jax.shard_map(local_step, mesh=mesh, in_specs=in_specs, out_specs=out_specs, check_vma=False)
```

```python
import functools

import jax
import jax.numpy as jnp
from jax import lax
from jax.experimental import pallas as pl
from jax.experimental.pallas import tpu as pltpu
from jax.sharding import PartitionSpec as P

TOK_AXES = ("dp", "row", "fsdp")
GROUP_AXES = ("row", "fsdp")
VMEM_BYTES = 67_000_000
MESH = pl.DeviceIdType.MESH

TILE1 = 768
TILE2 = 768
COLS = 256
MOVE = 128
SHARDS1 = 3
CHUNKS = 16
CORE_SUM = 3
ROW_SUM = 14
FORWARD = 12


def dot(lhs, rhs, lhs_dim, rhs_dim):
    return lax.dot_general(lhs, rhs, (((lhs_dim,), (rhs_dim,)), ((), ())), preferred_element_type=jnp.float32)


def wide_sum(a, b):
    return (a.astype(jnp.float32) + b.astype(jnp.float32)).astype(jnp.bfloat16)


def by_rows(rows, block, body):
    @pl.loop(0, rows // block)
    def _(i):
        body(pl.ds(pl.multiple_of(i * block, block), block))


def backward_tile(x_ref, dy_ref, w13_ref, w2_ref, z_ref, h_ref, dw_ref, first, put_dx):
    ff = h_ref.shape[1]
    for c in range(0, ff, COLS):
        gate = dot(x_ref[...], w13_ref[:, c : c + COLS], 1, 0)
        up = dot(x_ref[...], w13_ref[:, ff + c : ff + c + COLS], 1, 0)
        dh = dot(dy_ref[...], w2_ref[c : c + COLS, :], 1, 1)
        sig = jax.nn.sigmoid(gate)
        act = gate * sig
        h_ref[:, c : c + COLS] = (act * up).astype(jnp.bfloat16)
        z_ref[:, c : c + COLS] = (dh * up * (sig + act * (1.0 - sig))).astype(jnp.bfloat16)
        z_ref[:, ff + c : ff + c + COLS] = (dh * act).astype(jnp.bfloat16)
    dw13 = dot(x_ref[...], z_ref[...], 0, 0)
    for slab in range(2):
        dw_ref[slab] = jnp.where(first, 0.0, dw_ref[slab]) + dw13[:, slab * ff : (slab + 1) * ff]
    dw_ref[2] = jnp.where(first, 0.0, dw_ref[2]) + dot(dy_ref[...], h_ref[...], 0, 0)
    put_dx(dot(z_ref[...], w13_ref[...], 1, 1))


def first_kernel(
    x_ref, dy_ref, g_ref, w1_ref, w3_ref, w2_ref,
    dxp_ref, dws_ref, f1_ref, f3_ref, f2_ref, r_ref, c_ref,
    acc_ref, w13_ref, w2c_ref, w13s_ref, w2s_ref, z_ref, h_ref, send_ref, own_ref, core_ref, row_ref,
    w_loc, w_core, w_row, w_fwd, a_sem, b_sem, c_sem, out_sem, dx_sem,
):
    shard, tile = pl.program_id(0), pl.program_id(1)
    tiles = pl.num_programs(1)
    step = shard * tiles + tile
    steps = SHARDS1 * tiles
    dp, row, core = (lax.axis_index(a) for a in TOK_AXES)
    mate = (dp, row, 1 - core)
    across = (dp, 1 - row, core)
    replica = (1 - dp, row, core)
    ff = h_ref.shape[1]
    chunk = g_ref.shape[0]

    def push(src, dst, sems, k, to):
        return pltpu.make_async_remote_copy(
            src_ref=src, dst_ref=dst, send_sem=sems.at[0, k], recv_sem=sems.at[1, k], device_id=to, device_id_type=MESH
        )

    def slots(w13, w2):
        return w13.at[:, :ff], w13.at[:, ff:], w2

    now = slots(w13_ref, w2c_ref)
    near, far = (slots(w13s_ref.at[s], w2s_ref.at[s]) for s in range(2))

    weights = (w1_ref, w3_ref, w2_ref)
    local = [pltpu.make_async_copy(w, d, w_loc.at[k]) for k, (w, d) in enumerate(zip(weights, now))]
    to_mate = [push(w, d, w_core, k, mate) for k, (w, d) in enumerate(zip(weights, near))]
    to_row = [push(w, d, w_row, k, across) for k, (w, d) in enumerate(zip(weights, far))]
    forward = [push(w, d, w_fwd, k, mate) for k, (w, d) in enumerate(zip(far, (f1_ref, f3_ref, f2_ref)))]

    def rows_of(c):
        return pl.ds(pl.multiple_of(c * chunk, 16), chunk)

    def core_push(c):
        return push(send_ref.at[lax.rem(c, 2)], core_ref.at[:, rows_of(c), :], a_sem, c, mate)

    def row_push(c):
        return push(own_ref.at[1, rows_of(c), :], row_ref.at[rows_of(c), :], b_sem, c, across)

    def dp_push(c):
        return push(own_ref.at[0, rows_of(c), :], c_ref.at[rows_of(c), :], c_sem, c, replica)

    keep_sum = pltpu.make_async_copy(own_ref.at[0], r_ref, out_sem)

    def dx_rows(t):
        return pl.ds(pl.multiple_of(t * TILE1, TILE1), TILE1)

    def dx_out(t):
        return pltpu.make_async_copy(acc_ref.at[dx_rows(t), :], dxp_ref.at[dx_rows(t), :], dx_sem.at[t])

    def take(s):
        def rows13(sl):
            w13_ref[sl, :] = w13s_ref[s, sl, :]

        def rows2(sl):
            w2c_ref[sl, :] = w2s_ref[s, sl, :]

        by_rows(w13_ref.shape[0], 64, rows13)
        by_rows(ff, 64, rows2)

    def at(c, sl):
        return pl.ds(pl.multiple_of(c * chunk + sl.start, 16), sl.size)

    @pl.when(step == 0)
    def _():
        barrier = pltpu.get_barrier_semaphore()
        for to in (mate, across, replica):
            pl.semaphore_signal(barrier, inc=1, device_id=to, device_id_type=MESH)
        for copy in local:
            copy.start()
        pl.semaphore_wait(barrier, 3)
        for copy in (*to_row, *to_mate):
            copy.start()
        for copy in local:
            copy.wait()

    @pl.when(step == tiles)
    def _():
        for copy in to_mate:
            copy.wait_recv()
        take(0)

    @pl.when(step == 2 * tiles)
    def _():
        take(1)

    @pl.when(step == FORWARD)
    def _():
        for copy in to_row:
            copy.wait_recv()
        for copy in forward:
            copy.start()

    @pl.when((step >= 1) & (step <= CHUNKS))
    def _():
        core_push(step - 1).start()

    @pl.when(step < CHUNKS)
    def _():
        @pl.when(step >= 2)
        def _():
            core_push(step - 2).wait_send()

        def convert(sl):
            for k, r in enumerate((row, 1 - row)):
                mine = pl.ds(pl.multiple_of((2 * r + core) * ff, ff), ff)
                theirs = pl.ds(pl.multiple_of((2 * r + 1 - core) * ff, ff), ff)
                own_ref[k, at(step, sl), :] = g_ref[sl, mine].astype(jnp.bfloat16)
                send_ref[lax.rem(step, 2), k, sl, :] = g_ref[sl, theirs].astype(jnp.bfloat16)

        by_rows(chunk, 16, convert)

    @pl.when((step > CORE_SUM) & (step <= CORE_SUM + CHUNKS))
    def _():
        row_push(step - CORE_SUM - 1).start()

    @pl.when((step >= CORE_SUM) & (step < CORE_SUM + CHUNKS))
    def _():
        c = step - CORE_SUM
        core_push(c).wait_recv()

        def add(sl):
            for k in range(2):
                own_ref[k, at(c, sl), :] = wide_sum(own_ref[k, at(c, sl), :], core_ref[k, at(c, sl), :])

        by_rows(chunk, 16, add)

    @pl.when((step > ROW_SUM) & (step <= ROW_SUM + CHUNKS // 2))
    def _():
        for k in range(2):
            dp_push(2 * (step - ROW_SUM - 1) + k).start()

    @pl.when((step >= ROW_SUM) & (step < ROW_SUM + CHUNKS // 2))
    def _():
        for k in range(2):
            row_push(2 * (step - ROW_SUM) + k).wait_recv()

        def add(sl):
            sl = at(2 * (step - ROW_SUM), sl)
            own_ref[0, sl, :] = wide_sum(own_ref[0, sl, :], row_ref[sl, :])

        by_rows(2 * chunk, 32, add)

    @pl.when(step == ROW_SUM + CHUNKS // 2 + 1)
    def _():
        keep_sum.start()

    @pl.when(step > steps - tiles)
    def _():
        dx_out(tile - 1).start()

    def put_dx(dx):
        acc_ref[dx_rows(tile), :] = jnp.where(shard == 0, 0.0, acc_ref[dx_rows(tile), :]) + dx

    backward_tile(x_ref, dy_ref, w13_ref, w2c_ref, z_ref, h_ref, dws_ref.at[0], tile == 0, put_dx)

    @pl.when(step == steps - 1)
    def _():
        dx_out(tile).start()
        for copy in (*to_mate, *to_row):
            copy.wait_send()
        for copy in forward:
            copy.wait()
        core_push(CHUNKS - 2).wait_send()
        core_push(CHUNKS - 1).wait_send()
        for c in range(CHUNKS):
            row_push(c).wait_send()
            dp_push(c).wait()
        keep_sum.wait()
        for t in range(dxp_ref.shape[0] // TILE1):
            dx_out(t).wait()


def run_first(x, dy, weights, g):
    tokens, d = x.shape
    ff = weights[0].shape[1]
    g_rows, g_cols = g.shape
    chunk = g_rows // CHUNKS
    tiles = tokens // TILE1
    hbm = pl.BlockSpec(memory_space=pltpu.HBM)
    tok = pl.BlockSpec((TILE1, d), lambda s, j: (j, 0))
    bf16, f32, dma = jnp.bfloat16, jnp.float32, pltpu.SemaphoreType.DMA
    like = lambda v: jax.ShapeDtypeStruct(v.shape, v.dtype)
    return pl.pallas_call(
        first_kernel,
        grid=(SHARDS1, tiles),
        in_specs=[tok, tok, pl.BlockSpec((chunk, g_cols), lambda s, j: (jnp.minimum(s * tiles + j, CHUNKS - 1), 0)), hbm, hbm, hbm],
        out_specs=[hbm, pl.BlockSpec((1, 3, d, ff), lambda s, j: (s, 0, 0, 0)), hbm, hbm, hbm, hbm, hbm],
        out_shape=[
            jax.ShapeDtypeStruct((tokens, d), f32),
            jax.ShapeDtypeStruct((SHARDS1, 3, d, ff), f32),
            *[like(w) for w in weights],
            jax.ShapeDtypeStruct((g_rows, ff), bf16),
            jax.ShapeDtypeStruct((g_rows, ff), bf16),
        ],
        scratch_shapes=[
            pltpu.VMEM((tokens, d), f32),
            pltpu.VMEM((d, 2 * ff), bf16),
            pltpu.VMEM((ff, d), bf16),
            pltpu.VMEM((SHARDS1 - 1, d, 2 * ff), bf16),
            pltpu.VMEM((SHARDS1 - 1, ff, d), bf16),
            pltpu.VMEM((TILE1, 2 * ff), bf16),
            pltpu.VMEM((TILE1, ff), bf16),
            pltpu.VMEM((2, 2, chunk, ff), bf16),
            pltpu.VMEM((2, g_rows, ff), bf16),
            pltpu.VMEM((2, g_rows, ff), bf16),
            pltpu.VMEM((g_rows, ff), bf16),
            dma((3,)),
            dma((2, 3)),
            dma((2, 3)),
            dma((2, 3)),
            dma((2, CHUNKS)),
            dma((2, CHUNKS)),
            dma((2, CHUNKS)),
            dma(()),
            dma((tiles,)),
        ],
        compiler_params=pltpu.CompilerParams(
            vmem_limit_bytes=VMEM_BYTES, dimension_semantics=("arbitrary", "arbitrary"), collective_id=0, has_side_effects=True
        ),
        cost_estimate=pl.CostEstimate(flops=16 * SHARDS1 * tokens * d * ff, bytes_accessed=120_000_000, transcendentals=0),
        name="bwd_first",
    )(x, dy, g, *weights)


def last_kernel(
    x_ref, dy_ref, dxp_ref, dws_ref, w1_ref, w3_ref, w2_ref, r_ref, c_ref,
    dx_ref, next_ref, dw_ref,
    w13s_ref, z_ref, h_ref, dw_acc, move_ref, in_sem, move_sem, own_sem,
):
    tile, tiles = pl.program_id(0), pl.num_programs(0)
    row, core = lax.axis_index("row"), lax.axis_index("fsdp")
    ff = h_ref.shape[1]
    cols = [2 * row + core, 2 * row + 1 - core, 2 * (1 - row) + core, 2 * (1 - row) + 1 - core]
    lanes = [pl.ds(pl.multiple_of(q * ff, ff), ff) for q in cols]
    moves = dws_ref.shape[2] // MOVE

    def span(m):
        return pl.ds(pl.multiple_of(m * MOVE, MOVE), MOVE)

    def fetch(m):
        return pltpu.make_async_copy(dws_ref.at[:, :, span(m), :], move_ref.at[lax.rem(m, 2)], in_sem.at[lax.rem(m, 2)])

    def place(m):
        return [pltpu.make_async_copy(move_ref.at[lax.rem(m, 2), s], dw_ref.at[:, span(m), lanes[s]], move_sem.at[lax.rem(m, 2), s]) for s in range(SHARDS1)]

    @pl.when((tile >= 2) & (tile < moves + 2))
    def _():
        for copy in place(tile - 2):
            copy.wait()

    @pl.when(tile < moves)
    def _():
        fetch(tile).start()

    @pl.when((tile >= 1) & (tile < moves + 1))
    def _():
        fetch(tile - 1).wait()
        for copy in place(tile - 1):
            copy.start()

    @pl.when(tile == 0)
    def _():
        def join(sl):
            w13s_ref[sl, :ff] = w1_ref[sl, :]
            w13s_ref[sl, ff:] = w3_ref[sl, :]

        by_rows(w1_ref.shape[0], 64, join)

    next_ref[...] = r_ref[...].astype(jnp.float32) + c_ref[...].astype(jnp.float32)

    def put_dx(dx):
        dx_ref[...] = (dxp_ref[...] + dx).astype(jnp.bfloat16)

    backward_tile(x_ref, dy_ref, w13s_ref, w2_ref, z_ref, h_ref, dw_acc, tile == 0, put_dx)

    @pl.when(tile == tiles - 1)
    def _():
        own = pltpu.make_async_copy(dw_acc, dw_ref.at[:, :, lanes[3]], own_sem)
        own.start()
        own.wait()


def run_last(x, dy, dxp, dws, weights, mine, other):
    tokens, d = x.shape
    ff = weights[0].shape[1]
    tiles = tokens // TILE2
    g_rows = mine.shape[0]
    tok = pl.BlockSpec((TILE2, d), lambda j: (j, 0))
    full = lambda w: pl.BlockSpec(w.shape, lambda j: (0, 0))
    part = pl.BlockSpec((g_rows // tiles, ff), lambda j: (j, 0))
    return pl.pallas_call(
        last_kernel,
        grid=(tiles,),
        in_specs=[tok, tok, tok, pl.BlockSpec(memory_space=pltpu.HBM), *[full(w) for w in weights], part, part],
        out_specs=[tok, part, pl.BlockSpec(memory_space=pltpu.HBM)],
        out_shape=[
            jax.ShapeDtypeStruct((tokens, d), jnp.bfloat16),
            jax.ShapeDtypeStruct((g_rows, ff), jnp.float32),
            jax.ShapeDtypeStruct((3, d, 4 * ff), jnp.float32),
        ],
        scratch_shapes=[
            pltpu.VMEM((d, 2 * ff), jnp.bfloat16),
            pltpu.VMEM((TILE2, 2 * ff), jnp.bfloat16),
            pltpu.VMEM((TILE2, ff), jnp.bfloat16),
            pltpu.VMEM((3, d, ff), jnp.float32),
            pltpu.VMEM((2, SHARDS1, 3, MOVE, ff), jnp.float32),
            pltpu.SemaphoreType.DMA((2,)),
            pltpu.SemaphoreType.DMA((2, SHARDS1)),
            pltpu.SemaphoreType.DMA(()),
        ],
        compiler_params=pltpu.CompilerParams(vmem_limit_bytes=VMEM_BYTES, dimension_semantics=("arbitrary",)),
        cost_estimate=pl.CostEstimate(flops=16 * tokens * d * ff, bytes_accessed=90_000_000, transcendentals=0),
        name="bwd_last",
    )(x, dy, dxp, dws, *weights, mine, other)


def solution(mesh):
    def local_step(x_dev, dy_dev, gate_shard, up_shard, down_shard, g_dev):
        micro_count, tok_dev, d_model = x_dev.shape
        ff = gate_shard.shape[1]
        x, dy = (v.reshape(micro_count * tok_dev, d_model) for v in (x_dev, dy_dev))
        g = g_dev.reshape(3 * d_model, 4 * ff)
        dxp, dws, *far, mine, other = run_first(x, dy, (gate_shard, up_shard, down_shard), g)
        dx, grad_next, grad_layer = run_last(x, dy, dxp, dws, far, mine, other)
        return dx.reshape(micro_count, tok_dev, d_model), grad_next.reshape(3, d_model, ff), grad_layer[None]

    in_specs = (P(None, TOK_AXES, None), P(None, TOK_AXES, None), P(None, GROUP_AXES), P(None, GROUP_AXES), P(GROUP_AXES, None), P(TOK_AXES, None, None, None))
    out_specs = (P(None, TOK_AXES, None), P(None, None, GROUP_AXES), P(TOK_AXES, None, None, None))
    return jax.shard_map(local_step, mesh=mesh, in_specs=in_specs, out_specs=out_specs, check_vma=False)
```

```python
import functools

import jax
import jax.numpy as jnp
from jax import lax
from jax.experimental import pallas as pl
from jax.experimental.pallas import tpu as pltpu
from jax.sharding import PartitionSpec as P

TOK_AXES = ("dp", "row", "fsdp")
GROUP_AXES = ("row", "fsdp")
VMEM_BYTES = 67_000_000
MESH = pl.DeviceIdType.MESH

TILE1 = 768
TILE2 = 768
COLS = 256
MOVE = 128
SHARDS1 = 3
CHUNKS = 16
SPREAD = 6
CORE_SUM = 2
ROW_SUM = 6
FORWARD = 14


def dot(lhs, rhs, lhs_dim, rhs_dim):
    return lax.dot_general(lhs, rhs, (((lhs_dim,), (rhs_dim,)), ((), ())), preferred_element_type=jnp.float32)


def seldom(cond):
    return pl.loop(0, cond.astype(jnp.int32))


def by_rows(rows, block, body):
    @pl.loop(0, rows // block)
    def _(i):
        body(pl.ds(pl.multiple_of(i * block, block), block))


def backward_tile(x_ref, dy_ref, w13_ref, w2_ref, z_ref, h_ref, dw_ref, first, put_dx, before=(None,)):
    ff = h_ref.shape[1]
    for c in range(0, ff, COLS):
        gate = dot(x_ref[...], w13_ref[:, c : c + COLS], 1, 0)
        up = dot(x_ref[...], w13_ref[:, ff + c : ff + c + COLS], 1, 0)
        dh = dot(dy_ref[...], w2_ref[c : c + COLS, :], 1, 1)
        sig = jax.nn.sigmoid(gate)
        act = gate * sig
        h_ref[:, c : c + COLS] = (act * up).astype(jnp.bfloat16)
        z_ref[:, c : c + COLS] = (dh * up * (sig + act * (1.0 - sig))).astype(jnp.bfloat16)
        z_ref[:, ff + c : ff + c + COLS] = (dh * act).astype(jnp.bfloat16)
    dw13 = dot(x_ref[...], z_ref[...], 0, 0)
    for slab in range(2):
        dw_ref[slab] = jnp.where(first, 0.0, dw_ref[slab]) + dw13[:, slab * ff : (slab + 1) * ff]
    dw_ref[2] = jnp.where(first, 0.0, dw_ref[2]) + dot(dy_ref[...], h_ref[...], 0, 0)
    rows = z_ref.shape[0] // len(before)
    for k, call in enumerate(before):
        if call is not None:
            call()
        put_dx(k * rows, rows, dot(z_ref[k * rows : (k + 1) * rows, :], w13_ref[...], 1, 1))


def first_kernel(
    x_ref, dy_ref, g_ref, w1_ref, w3_ref, w2_ref,
    dxp_ref, dws_ref, f1_ref, f3_ref, f2_ref, r_ref, c_ref,
    acc_ref, dw_ref, w13_ref, w2c_ref, w13s_ref, w2s_ref, z_ref, h_ref, send_ref, own_ref, core_ref, row_ref,
    w_loc, w_core, w_row, w_rep, w_fwd, a_sem, b_sem, c_sem, out_sem, dx_sem, dw_sem,
):
    shard, tile = pl.program_id(0), pl.program_id(1)
    tiles = pl.num_programs(1)
    step = shard * tiles + tile
    steps = SHARDS1 * tiles
    dp, row, core = (lax.axis_index(a) for a in TOK_AXES)
    mate = (dp, row, 1 - core)
    across = (dp, 1 - row, core)
    replica = (1 - dp, row, core)
    ff = h_ref.shape[1]
    chunk = g_ref.shape[0]

    def push(src, dst, sems, k, to):
        return pltpu.make_async_remote_copy(
            src_ref=src, dst_ref=dst, send_sem=sems.at[0, k], recv_sem=sems.at[1, k], device_id=to, device_id_type=MESH
        )

    def slots(w13, w2):
        return w13.at[:, :ff], w13.at[:, ff:], w2

    now = slots(w13_ref, w2c_ref)
    near, far = (slots(w13s_ref.at[s], w2s_ref.at[s]) for s in range(2))

    weights = (w1_ref, w3_ref, w2_ref)
    local = [pltpu.make_async_copy(w, d, w_loc.at[k]) for k, (w, d) in enumerate(zip(weights, now))]
    to_mate = [push(w, d, w_core, k, mate) for k, (w, d) in enumerate(zip(weights, near))]
    forward = [push(w, d, w_fwd, k, mate) for k, (w, d) in enumerate(zip(far, (f1_ref, f3_ref, f2_ref)))]

    def half(v):
        rows = v.shape[0] // 2
        return v.at[pl.ds(pl.multiple_of(dp * rows, 16), rows), :]

    to_row = [push(half(w), half(d), w_row, k, across) for k, (w, d) in enumerate(zip(weights, far))]
    spread = [push(half(d), half(d), w_rep, k, replica) for k, d in enumerate(far)]

    def rows_of(c):
        return pl.ds(pl.multiple_of(c * chunk, 16), chunk)

    def core_push(c):
        return push(send_ref.at[lax.rem(c, 2)], core_ref.at[:, rows_of(c), :], a_sem, c, mate)

    def row_push(c):
        return push(own_ref.at[1, rows_of(c), :], row_ref.at[rows_of(c), :], b_sem, c, across)

    def dp_push(c):
        return push(own_ref.at[0, rows_of(c), :], c_ref.at[rows_of(c), :], c_sem, c, replica)

    keep_sum = pltpu.make_async_copy(own_ref.at[0], r_ref, out_sem)

    def dx_out(start, rows, k):
        sl = pl.ds(pl.multiple_of(start, 16), rows)
        return pltpu.make_async_copy(acc_ref.at[sl, :], dxp_ref.at[sl, :], dx_sem.at[k])

    third = TILE1 // 3
    dx_outs = [dx_out(t * TILE1, TILE1, t) for t in range(acc_ref.shape[0] // TILE1 - 1)]
    dx_lasts = [dx_out(acc_ref.shape[0] - TILE1 + k * third, third, len(dx_outs) + k) for k in range(3)]
    dw_outs = [pltpu.make_async_copy(dw_ref.at[k % 2], dws_ref.at[k], dw_sem.at[k]) for k in range(SHARDS1)]

    def take(s):
        def rows13(sl):
            w13_ref[sl, :] = w13s_ref[s, sl, :]

        def rows2(sl):
            w2c_ref[sl, :] = w2s_ref[s, sl, :]

        by_rows(w13_ref.shape[0], 128, rows13)
        by_rows(ff, 128, rows2)

    def at(c, sl):
        return pl.ds(pl.multiple_of(c * chunk + sl.start, 16), sl.size)

    turns = (0, SPREAD, tiles, FORWARD, 2 * tiles, ROW_SUM + CHUNKS + 1)

    @seldom(functools.reduce(jnp.logical_or, [step == t for t in turns]))
    def _(_):
        @pl.when(step == 0)
        def _():
            barrier = pltpu.get_barrier_semaphore()
            for to in (mate, across, replica):
                pl.semaphore_signal(barrier, inc=1, device_id=to, device_id_type=MESH)
            for copy in local:
                copy.start()
            pl.semaphore_wait(barrier, 3)
            for copy in (*to_row, *to_mate):
                copy.start()
            for copy in local:
                copy.wait()

        @pl.when(step == tiles)
        def _():
            for copy in to_mate:
                copy.wait_recv()
            take(0)
            dw_outs[0].start()

        @pl.when(step == 2 * tiles)
        def _():
            take(1)
            dw_outs[1].start()
            dw_outs[0].wait()

        @pl.when(step == SPREAD)
        def _():
            for copy in to_row:
                copy.wait_recv()
            for copy in spread:
                copy.start()

        @pl.when(step == FORWARD)
        def _():
            for copy in spread:
                copy.wait_recv()
            for copy in forward:
                copy.start()

        @pl.when(step == ROW_SUM + CHUNKS + 1)
        def _():
            keep_sum.start()

    @pl.when((step >= 1) & (step <= CHUNKS))
    def _():
        core_push(step - 1).start()

    @pl.when(step < CHUNKS)
    def _():
        @pl.when(step >= 2)
        def _():
            core_push(step - 2).wait_send()

        def convert(sl):
            for k, r in enumerate((row, 1 - row)):
                mine = pl.ds(pl.multiple_of((2 * r + core) * ff, ff), ff)
                theirs = pl.ds(pl.multiple_of((2 * r + 1 - core) * ff, ff), ff)
                own_ref[k, at(step, sl), :] = g_ref[sl, mine].astype(jnp.bfloat16)
                send_ref[lax.rem(step, 2), k, sl, :] = g_ref[sl, theirs].astype(jnp.bfloat16)

        by_rows(chunk, 48, convert)

    @pl.when((step > CORE_SUM) & (step <= CORE_SUM + CHUNKS))
    def _():
        row_push(step - CORE_SUM - 1).start()

    @pl.when((step >= CORE_SUM) & (step < CORE_SUM + CHUNKS))
    def _():
        c = step - CORE_SUM
        core_push(c).wait_recv()

        def add(sl):
            for k in range(2):
                own_ref[k, at(c, sl), :] = own_ref[k, at(c, sl), :] + core_ref[k, at(c, sl), :]

        by_rows(chunk, 48, add)

    @pl.when((step > ROW_SUM) & (step <= ROW_SUM + CHUNKS))
    def _():
        dp_push(step - ROW_SUM - 1).start()

    @pl.when((step >= ROW_SUM) & (step < ROW_SUM + CHUNKS))
    def _():
        c = step - ROW_SUM
        row_push(c).wait_recv()

        def add(sl):
            own_ref[0, at(c, sl), :] = own_ref[0, at(c, sl), :] + row_ref[at(c, sl), :]

        by_rows(chunk, 48, add)

    @pl.when(step > steps - tiles)
    def _():
        dx_out((tile - 1) * TILE1, TILE1, tile - 1).start()

    def put_dx(start, rows, dx):
        sl = pl.ds(pl.multiple_of(tile * TILE1 + start, 16), rows)
        acc_ref[sl, :] = jnp.where(shard == 0, 0.0, acc_ref[sl, :]) + dx

    def compute(**extra):
        backward_tile(x_ref, dy_ref, w13_ref, w2c_ref, z_ref, h_ref, dw_ref.at[lax.rem(shard, 2)], tile == 0, put_dx, **extra)

    @pl.when(step < steps - 1)
    def _():
        compute()

    @seldom(step == steps - 1)
    def _(_):
        compute(before=(None, dw_outs[2].start, dx_lasts[0].start))
        for copy in dx_lasts[1:]:
            copy.start()
        for copy in (*to_mate, *to_row, *spread):
            copy.wait_send()
        for copy in forward:
            copy.wait()
        core_push(CHUNKS - 2).wait_send()
        core_push(CHUNKS - 1).wait_send()
        for c in range(CHUNKS):
            row_push(c).wait_send()
            dp_push(c).wait()
        keep_sum.wait()
        for copy in (*dw_outs[1:], *dx_outs, *dx_lasts):
            copy.wait()


def run_first(x, dy, weights, g):
    tokens, d = x.shape
    ff = weights[0].shape[1]
    g_rows, g_cols = g.shape
    chunk = g_rows // CHUNKS
    tiles = tokens // TILE1
    hbm = pl.BlockSpec(memory_space=pltpu.HBM)
    tok = pl.BlockSpec((TILE1, d), lambda s, j: (j, 0))
    bf16, f32, dma = jnp.bfloat16, jnp.float32, pltpu.SemaphoreType.DMA
    like = lambda v: jax.ShapeDtypeStruct(v.shape, v.dtype)
    return pl.pallas_call(
        first_kernel,
        grid=(SHARDS1, tiles),
        in_specs=[tok, tok, pl.BlockSpec((chunk, g_cols), lambda s, j: (jnp.minimum(s * tiles + j, CHUNKS - 1), 0)), hbm, hbm, hbm],
        out_specs=[hbm, hbm, hbm, hbm, hbm, hbm, hbm],
        out_shape=[
            jax.ShapeDtypeStruct((tokens, d), f32),
            jax.ShapeDtypeStruct((SHARDS1, 3, d, ff), f32),
            *[like(w) for w in weights],
            jax.ShapeDtypeStruct((g_rows, ff), bf16),
            jax.ShapeDtypeStruct((g_rows, ff), bf16),
        ],
        scratch_shapes=[
            pltpu.VMEM((tokens, d), f32),
            pltpu.VMEM((2, 3, d, ff), f32),
            pltpu.VMEM((d, 2 * ff), bf16),
            pltpu.VMEM((ff, d), bf16),
            pltpu.VMEM((SHARDS1 - 1, d, 2 * ff), bf16),
            pltpu.VMEM((SHARDS1 - 1, ff, d), bf16),
            pltpu.VMEM((TILE1, 2 * ff), bf16),
            pltpu.VMEM((TILE1, ff), bf16),
            pltpu.VMEM((2, 2, chunk, ff), bf16),
            pltpu.VMEM((2, g_rows, ff), bf16),
            pltpu.VMEM((2, g_rows, ff), bf16),
            pltpu.VMEM((g_rows, ff), bf16),
            dma((3,)),
            dma((2, 3)),
            dma((2, 3)),
            dma((2, 3)),
            dma((2, 3)),
            dma((2, CHUNKS)),
            dma((2, CHUNKS)),
            dma((2, CHUNKS)),
            dma(()),
            dma((tiles + 2,)),
            dma((SHARDS1,)),
        ],
        compiler_params=pltpu.CompilerParams(
            vmem_limit_bytes=VMEM_BYTES, dimension_semantics=("arbitrary", "arbitrary"), collective_id=0, has_side_effects=True
        ),
        cost_estimate=pl.CostEstimate(flops=16 * SHARDS1 * tokens * d * ff, bytes_accessed=120_000_000, transcendentals=0),
        name="bwd_first",
    )(x, dy, g, *weights)


def last_kernel(
    x_ref, dy_ref, dxp_ref, dws_ref, w1_ref, w3_ref, w2_ref, r_ref, c_ref,
    dx_ref, next_ref, dw_ref,
    w13s_ref, z_ref, h_ref, dw_acc, move_ref, in_sem, move_sem, own_sem,
):
    tile, tiles = pl.program_id(0), pl.num_programs(0)
    row, core = lax.axis_index("row"), lax.axis_index("fsdp")
    ff = h_ref.shape[1]
    cols = [2 * row + core, 2 * row + 1 - core, 2 * (1 - row) + core, 2 * (1 - row) + 1 - core]
    lanes = [pl.ds(pl.multiple_of(q * ff, ff), ff) for q in cols]
    moves = dws_ref.shape[2] // MOVE

    def span(m):
        return pl.ds(pl.multiple_of(m * MOVE, MOVE), MOVE)

    def fetch(m):
        return pltpu.make_async_copy(dws_ref.at[:, :, span(m), :], move_ref.at[lax.rem(m, 2)], in_sem.at[lax.rem(m, 2)])

    def place(m):
        return [pltpu.make_async_copy(move_ref.at[lax.rem(m, 2), s], dw_ref.at[:, span(m), lanes[s]], move_sem.at[lax.rem(m, 2), s]) for s in range(SHARDS1)]

    @pl.when((tile >= 2) & (tile < moves + 2))
    def _():
        for copy in place(tile - 2):
            copy.wait()

    @pl.when(tile < moves)
    def _():
        fetch(tile).start()

    @pl.when((tile >= 1) & (tile < moves + 1))
    def _():
        fetch(tile - 1).wait()
        for copy in place(tile - 1):
            copy.start()

    @pl.when(tile == 0)
    def _():
        def join(sl):
            w13s_ref[sl, :ff] = w1_ref[sl, :]
            w13s_ref[sl, ff:] = w3_ref[sl, :]

        by_rows(w1_ref.shape[0], 256, join)

    next_ref[...] = r_ref[...].astype(jnp.float32) + c_ref[...].astype(jnp.float32)

    def put_dx(start, rows, dx):
        sl = slice(start, start + rows)
        dx_ref[sl, :] = (dxp_ref[sl, :] + dx).astype(jnp.bfloat16)

    def compute(**extra):
        backward_tile(x_ref, dy_ref, w13s_ref, w2_ref, z_ref, h_ref, dw_acc, tile == 0, put_dx, **extra)

    @pl.when(tile < tiles - 1)
    def _():
        compute()

    @pl.when(tile == tiles - 1)
    def _():
        own = pltpu.make_async_copy(dw_acc, dw_ref.at[:, :, lanes[3]], own_sem)
        compute(before=(None, own.start))
        own.wait()


def run_last(x, dy, dxp, dws, weights, mine, other):
    tokens, d = x.shape
    ff = weights[0].shape[1]
    tiles = tokens // TILE2
    g_rows = mine.shape[0]
    tok = pl.BlockSpec((TILE2, d), lambda j: (j, 0))
    full = lambda w: pl.BlockSpec(w.shape, lambda j: (0, 0))
    part = pl.BlockSpec((g_rows // tiles, ff), lambda j: (j, 0))
    return pl.pallas_call(
        last_kernel,
        grid=(tiles,),
        in_specs=[tok, tok, tok, pl.BlockSpec(memory_space=pltpu.HBM), *[full(w) for w in weights], part, part],
        out_specs=[tok, part, pl.BlockSpec(memory_space=pltpu.HBM)],
        out_shape=[
            jax.ShapeDtypeStruct((tokens, d), jnp.bfloat16),
            jax.ShapeDtypeStruct((g_rows, ff), jnp.float32),
            jax.ShapeDtypeStruct((3, d, 4 * ff), jnp.float32),
        ],
        scratch_shapes=[
            pltpu.VMEM((d, 2 * ff), jnp.bfloat16),
            pltpu.VMEM((TILE2, 2 * ff), jnp.bfloat16),
            pltpu.VMEM((TILE2, ff), jnp.bfloat16),
            pltpu.VMEM((3, d, ff), jnp.float32),
            pltpu.VMEM((2, SHARDS1, 3, MOVE, ff), jnp.float32),
            pltpu.SemaphoreType.DMA((2,)),
            pltpu.SemaphoreType.DMA((2, SHARDS1)),
            pltpu.SemaphoreType.DMA(()),
        ],
        compiler_params=pltpu.CompilerParams(vmem_limit_bytes=VMEM_BYTES, dimension_semantics=("arbitrary",)),
        cost_estimate=pl.CostEstimate(flops=16 * tokens * d * ff, bytes_accessed=90_000_000, transcendentals=0),
        name="bwd_last",
    )(x, dy, dxp, dws, *weights, mine, other)


def solution(mesh):
    def local_step(x_dev, dy_dev, gate_shard, up_shard, down_shard, g_dev):
        micro_count, tok_dev, d_model = x_dev.shape
        ff = gate_shard.shape[1]
        x, dy = (v.reshape(micro_count * tok_dev, d_model) for v in (x_dev, dy_dev))
        g = g_dev.reshape(3 * d_model, 4 * ff)
        dxp, dws, *far, mine, other = run_first(x, dy, (gate_shard, up_shard, down_shard), g)
        dx, grad_next, grad_layer = run_last(x, dy, dxp, dws, far, mine, other)
        return dx.reshape(micro_count, tok_dev, d_model), grad_next.reshape(3, d_model, ff), grad_layer[None]

    in_specs = (P(None, TOK_AXES, None), P(None, TOK_AXES, None), P(None, GROUP_AXES), P(None, GROUP_AXES), P(GROUP_AXES, None), P(TOK_AXES, None, None, None))
    out_specs = (P(None, TOK_AXES, None), P(None, None, GROUP_AXES), P(TOK_AXES, None, None, None))
    return jax.shard_map(local_step, mesh=mesh, in_specs=in_specs, out_specs=out_specs, check_vma=False)
```

```python
import functools

import jax
import jax.numpy as jnp
from jax import lax
from jax.experimental import pallas as pl
from jax.experimental.pallas import tpu as pltpu
from jax.sharding import PartitionSpec as P

TOK_AXES = ("dp", "row", "fsdp")
GROUP_AXES = ("row", "fsdp")
VMEM_BYTES = 67_000_000
MESH = pl.DeviceIdType.MESH

TILE1 = 768
TILE2 = 768
COLS = 256
MOVE = 128
SHARDS1 = 3
CHUNKS = 16
SPREAD = 7
CORE_SUM = 2
ROW_SUM = 7
FORWARD = 14


def dot(lhs, rhs, lhs_dim, rhs_dim):
    return lax.dot_general(lhs, rhs, (((lhs_dim,), (rhs_dim,)), ((), ())), preferred_element_type=jnp.float32)


def seldom(cond):
    return pl.loop(0, cond.astype(jnp.int32))


def by_rows(rows, block, body):
    @pl.loop(0, rows // block)
    def _(i):
        body(pl.ds(pl.multiple_of(i * block, block), block))


def backward_tile(x_ref, dy_ref, w13_ref, w2_ref, z_ref, h_ref, dw_ref, first, put_dx, aside, before=(None,)):
    ff = h_ref.shape[1]
    for c in range(0, ff, COLS):
        gate = dot(x_ref[...], w13_ref[:, c : c + COLS], 1, 0)
        up = dot(x_ref[...], w13_ref[:, ff + c : ff + c + COLS], 1, 0)
        dh = dot(dy_ref[...], w2_ref[c : c + COLS, :], 1, 1)
        sig = jax.nn.sigmoid(gate)
        act = gate * sig
        h_ref[:, c : c + COLS] = (act * up).astype(jnp.bfloat16)
        z_ref[:, c : c + COLS] = (dh * up * (sig + act * (1.0 - sig))).astype(jnp.bfloat16)
        z_ref[:, ff + c : ff + c + COLS] = (dh * act).astype(jnp.bfloat16)
    dw13 = dot(x_ref[...], z_ref[...], 0, 0)
    for slab in range(2):
        dw_ref[slab] = jnp.where(first, 0.0, dw_ref[slab]) + dw13[:, slab * ff : (slab + 1) * ff]
    dw_ref[2] = jnp.where(first, 0.0, dw_ref[2]) + dot(dy_ref[...], h_ref[...], 0, 0)
    aside()
    rows = z_ref.shape[0] // len(before)
    for k, call in enumerate(before):
        if call is not None:
            call()
        put_dx(k * rows, rows, dot(z_ref[k * rows : (k + 1) * rows, :], w13_ref[...], 1, 1))


def first_kernel(
    x_ref, dy_ref, g_ref, w1_ref, w3_ref, w2_ref,
    dxp_ref, dws_ref, f1_ref, f3_ref, f2_ref, r_ref, c_ref,
    acc_ref, dw_ref, w13_ref, w2c_ref, w13s_ref, w2s_ref, z_ref, h_ref, send_ref, own_ref, core_ref, row_ref,
    w_loc, w_core, w_row, w_rep, w_fwd, a_sem, b_sem, c_sem, out_sem, dx_sem, dw_sem,
):
    shard, tile = pl.program_id(0), pl.program_id(1)
    tiles = pl.num_programs(1)
    step = shard * tiles + tile
    steps = SHARDS1 * tiles
    dp, row, core = (lax.axis_index(a) for a in TOK_AXES)
    mate = (dp, row, 1 - core)
    across = (dp, 1 - row, core)
    replica = (1 - dp, row, core)
    ff = h_ref.shape[1]
    chunk = g_ref.shape[0]

    def push(src, dst, sems, k, to):
        return pltpu.make_async_remote_copy(
            src_ref=src, dst_ref=dst, send_sem=sems.at[0, k], recv_sem=sems.at[1, k], device_id=to, device_id_type=MESH
        )

    def slots(w13, w2):
        return w13.at[:, :ff], w13.at[:, ff:], w2

    now = slots(w13_ref, w2c_ref)
    near, far = (slots(w13s_ref.at[s], w2s_ref.at[s]) for s in range(2))

    weights = (w1_ref, w3_ref, w2_ref)
    local = [pltpu.make_async_copy(w, d, w_loc.at[k]) for k, (w, d) in enumerate(zip(weights, now))]
    to_mate = [push(w, d, w_core, k, mate) for k, (w, d) in enumerate(zip(weights, near))]
    forward = [push(w, d, w_fwd, k, mate) for k, (w, d) in enumerate(zip(far, (f1_ref, f3_ref, f2_ref)))]

    def half(v):
        rows = v.shape[0] // 2
        return v.at[pl.ds(pl.multiple_of(dp * rows, 16), rows), :]

    to_row = [push(half(w), half(d), w_row, k, across) for k, (w, d) in enumerate(zip(weights, far))]
    spread = [push(half(d), half(d), w_rep, k, replica) for k, d in enumerate(far)]

    def rows_of(c):
        return pl.ds(pl.multiple_of(c * chunk, 16), chunk)

    def core_push(c):
        return push(send_ref.at[lax.rem(c, 2)], core_ref.at[:, rows_of(c), :], a_sem, c, mate)

    def row_push(c):
        return push(own_ref.at[1, rows_of(c), :], row_ref.at[rows_of(c), :], b_sem, c, across)

    def dp_push(c):
        return push(own_ref.at[0, rows_of(c), :], c_ref.at[rows_of(c), :], c_sem, c, replica)

    keep_sum = pltpu.make_async_copy(own_ref.at[0, : r_ref.shape[0], :], r_ref, out_sem)

    def dx_out(start, rows, k):
        sl = pl.ds(pl.multiple_of(start, 16), rows)
        return pltpu.make_async_copy(acc_ref.at[sl, :], dxp_ref.at[sl, :], dx_sem.at[k])

    third = TILE1 // 3
    dx_outs = [dx_out(t * TILE1, TILE1, t) for t in range(acc_ref.shape[0] // TILE1 - 1)]
    dx_lasts = [dx_out(acc_ref.shape[0] - TILE1 + k * third, third, len(dx_outs) + k) for k in range(3)]
    dw_outs = [pltpu.make_async_copy(dw_ref.at[k % 2], dws_ref.at[k], dw_sem.at[k]) for k in range(SHARDS1)]

    def take(s):
        def rows13(sl):
            w13_ref[sl, :] = w13s_ref[s, sl, :]

        def rows2(sl):
            w2c_ref[sl, :] = w2s_ref[s, sl, :]

        by_rows(w13_ref.shape[0], 128, rows13)
        by_rows(ff, 128, rows2)

    turns = (0, 1, SPREAD, tiles, FORWARD, 2 * tiles, ROW_SUM + CHUNKS)

    @seldom(functools.reduce(jnp.logical_or, [step == t for t in turns]))
    def _(_):
        barrier = pltpu.get_barrier_semaphore()

        @pl.when(step == 0)
        def _():
            for to in (mate, across, replica):
                pl.semaphore_signal(barrier, inc=1, device_id=to, device_id_type=MESH)
            for copy in local:
                copy.start()
            for copy in local:
                copy.wait()

        @pl.when(step == 1)
        def _():
            pl.semaphore_wait(barrier, 3)
            for copy in (*to_row, *to_mate):
                copy.start()

        @pl.when(step == tiles)
        def _():
            for copy in to_mate:
                copy.wait_recv()
            take(0)
            dw_outs[0].start()

        @pl.when(step == 2 * tiles)
        def _():
            take(1)
            dw_outs[1].start()
            dw_outs[0].wait()

        @pl.when(step == SPREAD)
        def _():
            for copy in to_row:
                copy.wait_recv()
            for copy in spread:
                copy.start()

        @pl.when(step == FORWARD)
        def _():
            for copy in spread:
                copy.wait_recv()
            for copy in forward:
                copy.start()

        @pl.when(step == ROW_SUM + CHUNKS)
        def _():
            keep_sum.start()

    def chunk_at(lag):
        c = step - lag
        return jnp.where((c >= 0) & (c < CHUNKS), c, CHUNKS)

    def has_chunk(lag):
        return (step >= lag) & (step < lag + CHUNKS)

    @pl.when(has_chunk(1))
    def _():
        core_push(step - 1).start()

    @pl.when(has_chunk(2))
    def _():
        core_push(step - 2).wait_send()

    @pl.when(has_chunk(CORE_SUM + 1))
    def _():
        row_push(step - CORE_SUM - 1).start()

    @pl.when(has_chunk(CORE_SUM))
    def _():
        core_push(step - CORE_SUM).wait_recv()

    @pl.when(has_chunk(ROW_SUM + 1))
    def _():
        dp_push(step - ROW_SUM - 1).start()

    @pl.when(has_chunk(ROW_SUM))
    def _():
        row_push(step - ROW_SUM).wait_recv()

    def reduce_chunks():
        now, summed, done = rows_of(chunk_at(0)), rows_of(chunk_at(CORE_SUM)), rows_of(chunk_at(ROW_SUM))
        own_ref[0, done, :] = own_ref[0, done, :] + row_ref[done, :]
        own_ref[:, summed, :] = own_ref[:, summed, :] + core_ref[:, summed, :]
        for k, r in enumerate((row, 1 - row)):
            mine = pl.ds(pl.multiple_of((2 * r + core) * ff, ff), ff)
            theirs = pl.ds(pl.multiple_of((2 * r + 1 - core) * ff, ff), ff)
            own_ref[k, now, :] = g_ref[:, mine].astype(jnp.bfloat16)
            send_ref[lax.rem(step, 2), k] = g_ref[:, theirs].astype(jnp.bfloat16)

    @pl.when(step > steps - tiles)
    def _():
        dx_out((tile - 1) * TILE1, TILE1, tile - 1).start()

    def put_dx(start, rows, dx):
        sl = pl.ds(pl.multiple_of(tile * TILE1 + start, 16), rows)
        acc_ref[sl, :] = jnp.where(shard == 0, 0.0, acc_ref[sl, :]) + dx

    def compute(**extra):
        backward_tile(x_ref, dy_ref, w13_ref, w2c_ref, z_ref, h_ref, dw_ref.at[lax.rem(shard, 2)], tile == 0, put_dx, reduce_chunks, **extra)

    @pl.when(step < steps - 1)
    def _():
        compute()

    @seldom(step == steps - 1)
    def _(_):
        compute(before=(None, dw_outs[2].start, dx_lasts[0].start))
        for copy in dx_lasts[1:]:
            copy.start()
        for copy in (*to_mate, *to_row, *spread):
            copy.wait_send()
        for copy in forward:
            copy.wait()
        for c in range(CHUNKS):
            row_push(c).wait_send()
            dp_push(c).wait()
        keep_sum.wait()
        for copy in (*dw_outs[1:], *dx_outs, *dx_lasts):
            copy.wait()


def run_first(x, dy, weights, g):
    tokens, d = x.shape
    ff = weights[0].shape[1]
    g_rows, g_cols = g.shape
    chunk = g_rows // CHUNKS
    tiles = tokens // TILE1
    hbm = pl.BlockSpec(memory_space=pltpu.HBM)
    tok = pl.BlockSpec((TILE1, d), lambda s, j: (j, 0))
    bf16, f32, dma = jnp.bfloat16, jnp.float32, pltpu.SemaphoreType.DMA
    like = lambda v: jax.ShapeDtypeStruct(v.shape, v.dtype)
    return pl.pallas_call(
        first_kernel,
        grid=(SHARDS1, tiles),
        in_specs=[tok, tok, pl.BlockSpec((chunk, g_cols), lambda s, j: (jnp.minimum(s * tiles + j, CHUNKS - 1), 0)), hbm, hbm, hbm],
        out_specs=[hbm, hbm, hbm, hbm, hbm, hbm, hbm],
        out_shape=[
            jax.ShapeDtypeStruct((tokens, d), f32),
            jax.ShapeDtypeStruct((SHARDS1, 3, d, ff), f32),
            *[like(w) for w in weights],
            jax.ShapeDtypeStruct((g_rows, ff), bf16),
            jax.ShapeDtypeStruct((g_rows, ff), bf16),
        ],
        scratch_shapes=[
            pltpu.VMEM((tokens, d), f32),
            pltpu.VMEM((2, 3, d, ff), f32),
            pltpu.VMEM((d, 2 * ff), bf16),
            pltpu.VMEM((ff, d), bf16),
            pltpu.VMEM((SHARDS1 - 1, d, 2 * ff), bf16),
            pltpu.VMEM((SHARDS1 - 1, ff, d), bf16),
            pltpu.VMEM((TILE1, 2 * ff), bf16),
            pltpu.VMEM((TILE1, ff), bf16),
            pltpu.VMEM((2, 2, chunk, ff), bf16),
            pltpu.VMEM((2, g_rows + chunk, ff), bf16),
            pltpu.VMEM((2, g_rows + chunk, ff), bf16),
            pltpu.VMEM((g_rows + chunk, ff), bf16),
            dma((3,)),
            dma((2, 3)),
            dma((2, 3)),
            dma((2, 3)),
            dma((2, 3)),
            dma((2, CHUNKS)),
            dma((2, CHUNKS)),
            dma((2, CHUNKS)),
            dma(()),
            dma((tiles + 2,)),
            dma((SHARDS1,)),
        ],
        compiler_params=pltpu.CompilerParams(
            vmem_limit_bytes=VMEM_BYTES, dimension_semantics=("arbitrary", "arbitrary"), collective_id=0, has_side_effects=True
        ),
        cost_estimate=pl.CostEstimate(flops=16 * SHARDS1 * tokens * d * ff, bytes_accessed=120_000_000, transcendentals=0),
        name="bwd_first",
    )(x, dy, g, *weights)


def last_kernel(
    x_ref, dy_ref, dxp_ref, dws_ref, w1_ref, w3_ref, w2_ref, r_ref, c_ref,
    dx_ref, next_ref, dw_ref,
    w13s_ref, z_ref, h_ref, dw_acc, move_ref, in_sem, move_sem, own_sem,
):
    tile, tiles = pl.program_id(0), pl.num_programs(0)
    row, core = lax.axis_index("row"), lax.axis_index("fsdp")
    ff = h_ref.shape[1]
    cols = [2 * row + core, 2 * row + 1 - core, 2 * (1 - row) + core, 2 * (1 - row) + 1 - core]
    lanes = [pl.ds(pl.multiple_of(q * ff, ff), ff) for q in cols]
    moves = dws_ref.shape[2] // MOVE

    def span(m):
        return pl.ds(pl.multiple_of(m * MOVE, MOVE), MOVE)

    def fetch(m):
        return pltpu.make_async_copy(dws_ref.at[:, :, span(m), :], move_ref.at[lax.rem(m, 2)], in_sem.at[lax.rem(m, 2)])

    def place(m):
        return [pltpu.make_async_copy(move_ref.at[lax.rem(m, 2), s], dw_ref.at[:, span(m), lanes[s]], move_sem.at[lax.rem(m, 2), s]) for s in range(SHARDS1)]

    @pl.when((tile >= 2) & (tile < moves + 2))
    def _():
        for copy in place(tile - 2):
            copy.wait()

    @pl.when(tile < moves)
    def _():
        fetch(tile).start()

    @pl.when((tile >= 1) & (tile < moves + 1))
    def _():
        fetch(tile - 1).wait()
        for copy in place(tile - 1):
            copy.start()

    @pl.when(tile == 0)
    def _():
        def join(sl):
            w13s_ref[sl, :ff] = w1_ref[sl, :]
            w13s_ref[sl, ff:] = w3_ref[sl, :]

        by_rows(w1_ref.shape[0], 256, join)


    def put_dx(start, rows, dx):
        sl = slice(start, start + rows)
        dx_ref[sl, :] = (dxp_ref[sl, :] + dx).astype(jnp.bfloat16)

    def add_replicas():
        next_ref[...] = r_ref[...].astype(jnp.float32) + c_ref[...].astype(jnp.float32)

    def compute(**extra):
        backward_tile(x_ref, dy_ref, w13s_ref, w2_ref, z_ref, h_ref, dw_acc, tile == 0, put_dx, add_replicas, **extra)

    @pl.when(tile < tiles - 1)
    def _():
        compute()

    @pl.when(tile == tiles - 1)
    def _():
        own = pltpu.make_async_copy(dw_acc, dw_ref.at[:, :, lanes[3]], own_sem)
        compute(before=(None, own.start))
        own.wait()


def run_last(x, dy, dxp, dws, weights, mine, other):
    tokens, d = x.shape
    ff = weights[0].shape[1]
    tiles = tokens // TILE2
    g_rows = mine.shape[0]
    tok = pl.BlockSpec((TILE2, d), lambda j: (j, 0))
    full = lambda w: pl.BlockSpec(w.shape, lambda j: (0, 0))
    part = pl.BlockSpec((g_rows // tiles, ff), lambda j: (j, 0))
    return pl.pallas_call(
        last_kernel,
        grid=(tiles,),
        in_specs=[tok, tok, tok, pl.BlockSpec(memory_space=pltpu.HBM), *[full(w) for w in weights], part, part],
        out_specs=[tok, part, pl.BlockSpec(memory_space=pltpu.HBM)],
        out_shape=[
            jax.ShapeDtypeStruct((tokens, d), jnp.bfloat16),
            jax.ShapeDtypeStruct((g_rows, ff), jnp.float32),
            jax.ShapeDtypeStruct((3, d, 4 * ff), jnp.float32),
        ],
        scratch_shapes=[
            pltpu.VMEM((d, 2 * ff), jnp.bfloat16),
            pltpu.VMEM((TILE2, 2 * ff), jnp.bfloat16),
            pltpu.VMEM((TILE2, ff), jnp.bfloat16),
            pltpu.VMEM((3, d, ff), jnp.float32),
            pltpu.VMEM((2, SHARDS1, 3, MOVE, ff), jnp.float32),
            pltpu.SemaphoreType.DMA((2,)),
            pltpu.SemaphoreType.DMA((2, SHARDS1)),
            pltpu.SemaphoreType.DMA(()),
        ],
        compiler_params=pltpu.CompilerParams(vmem_limit_bytes=VMEM_BYTES, dimension_semantics=("arbitrary",)),
        cost_estimate=pl.CostEstimate(flops=16 * tokens * d * ff, bytes_accessed=90_000_000, transcendentals=0),
        name="bwd_last",
    )(x, dy, dxp, dws, *weights, mine, other)


def solution(mesh):
    def local_step(x_dev, dy_dev, gate_shard, up_shard, down_shard, g_dev):
        micro_count, tok_dev, d_model = x_dev.shape
        ff = gate_shard.shape[1]
        x, dy = (v.reshape(micro_count * tok_dev, d_model) for v in (x_dev, dy_dev))
        g = g_dev.reshape(3 * d_model, 4 * ff)
        dxp, dws, *far, mine, other = run_first(x, dy, (gate_shard, up_shard, down_shard), g)
        dx, grad_next, grad_layer = run_last(x, dy, dxp, dws, far, mine, other)
        return dx.reshape(micro_count, tok_dev, d_model), grad_next.reshape(3, d_model, ff), grad_layer[None]

    in_specs = (P(None, TOK_AXES, None), P(None, TOK_AXES, None), P(None, GROUP_AXES), P(None, GROUP_AXES), P(GROUP_AXES, None), P(TOK_AXES, None, None, None))
    out_specs = (P(None, TOK_AXES, None), P(None, None, GROUP_AXES), P(TOK_AXES, None, None, None))
    return jax.shard_map(local_step, mesh=mesh, in_specs=in_specs, out_specs=out_specs, check_vma=False)
```

```python
import functools

import jax
import jax.numpy as jnp
from jax import lax
from jax.experimental import pallas as pl
from jax.experimental.pallas import tpu as pltpu
from jax.sharding import PartitionSpec as P

TOK_AXES = ("dp", "row", "fsdp")
GROUP_AXES = ("row", "fsdp")
VMEM_BYTES = 67_000_000
MESH = pl.DeviceIdType.MESH

TILE1 = 768
TILE2 = 768
COLS = 256
MOVE = 128
SHARDS1 = 3
CHUNKS = 16
SPREAD = 7
CORE_SUM = 2
ROW_SUM = 7
FORWARD = 14


def dot(lhs, rhs, lhs_dim, rhs_dim):
    return lax.dot_general(lhs, rhs, (((lhs_dim,), (rhs_dim,)), ((), ())), preferred_element_type=jnp.float32)


def seldom(cond):
    return pl.loop(0, cond.astype(jnp.int32))


def by_rows(rows, block, body):
    @pl.loop(0, rows // block)
    def _(i):
        body(pl.ds(pl.multiple_of(i * block, block), block))


def backward_tile(x_ref, dy_ref, w13_ref, w2_ref, z_ref, h_ref, dw_ref, first, put_dx, aside, before=(None,)):
    ff = h_ref.shape[1]
    for c in range(0, ff, COLS):
        gate = dot(x_ref[...], w13_ref[:, c : c + COLS], 1, 0)
        up = dot(x_ref[...], w13_ref[:, ff + c : ff + c + COLS], 1, 0)
        dh = dot(dy_ref[...], w2_ref[c : c + COLS, :], 1, 1)
        sig = jax.nn.sigmoid(gate)
        act = gate * sig
        h_ref[:, c : c + COLS] = (act * up).astype(jnp.bfloat16)
        z_ref[:, c : c + COLS] = (dh * up * (sig + act * (1.0 - sig))).astype(jnp.bfloat16)
        z_ref[:, ff + c : ff + c + COLS] = (dh * act).astype(jnp.bfloat16)
    dw13 = dot(x_ref[...], z_ref[...], 0, 0)
    for slab in range(2):
        dw_ref[slab] = jnp.where(first, 0.0, dw_ref[slab]) + dw13[:, slab * ff : (slab + 1) * ff]
    dw_ref[2] = jnp.where(first, 0.0, dw_ref[2]) + dot(dy_ref[...], h_ref[...], 0, 0)
    aside()
    rows = z_ref.shape[0] // len(before)
    for k, call in enumerate(before):
        if call is not None:
            call()
        put_dx(k * rows, rows, dot(z_ref[k * rows : (k + 1) * rows, :], w13_ref[...], 1, 1))


def first_kernel(
    x_ref, dy_ref, g_ref, w1_ref, w3_ref, w2_ref,
    dxp_ref, dws_ref, f13_ref, f2_ref, r_ref, c_ref,
    acc_ref, dw_ref, w13_ref, w2c_ref, w13s_ref, w2s_ref, z_ref, h_ref, send_ref, own_ref, core_ref, row_ref,
    w_core, w_row, w_rep, w_fwd, a_sem, b_sem, c_sem, out_sem, dx_sem, dw_sem,
):
    shard, tile = pl.program_id(0), pl.program_id(1)
    tiles = pl.num_programs(1)
    step = shard * tiles + tile
    steps = SHARDS1 * tiles
    dp, row, core = (lax.axis_index(a) for a in TOK_AXES)
    mate = (dp, row, 1 - core)
    across = (dp, 1 - row, core)
    replica = (1 - dp, row, core)
    ff = h_ref.shape[1]
    chunk = g_ref.shape[0]

    def push(src, dst, sems, k, to):
        return pltpu.make_async_remote_copy(
            src_ref=src, dst_ref=dst, send_sem=sems.at[0, k], recv_sem=sems.at[1, k], device_id=to, device_id_type=MESH
        )

    def slots(w13, w2):
        return w13.at[:, :ff], w13.at[:, ff:], w2

    near, far = (slots(w13s_ref.at[s], w2s_ref.at[s]) for s in range(2))

    weights = (w1_ref, w3_ref, w2_ref)
    to_mate = [push(w, d, w_core, k, mate) for k, (w, d) in enumerate(zip(weights, near))]
    forward = [push(w, d, w_fwd, k, mate) for k, (w, d) in enumerate(((w13s_ref.at[1], f13_ref), (w2s_ref.at[1], f2_ref)))]

    def half(v):
        rows = v.shape[0] // 2
        return v.at[pl.ds(pl.multiple_of(dp * rows, 16), rows), :]

    to_row = [push(half(w), half(d), w_row, k, across) for k, (w, d) in enumerate(zip(weights, far))]
    spread = [push(half(d), half(d), w_rep, k, replica) for k, d in enumerate(far)]

    def rows_of(c):
        return pl.ds(pl.multiple_of(c * chunk, 16), chunk)

    def core_push(c):
        return push(send_ref.at[lax.rem(c, 2)], core_ref.at[:, rows_of(c), :], a_sem, c, mate)

    def row_push(c):
        return push(own_ref.at[1, rows_of(c), :], row_ref.at[rows_of(c), :], b_sem, c, across)

    def dp_push(c):
        return push(own_ref.at[0, rows_of(c), :], c_ref.at[rows_of(c), :], c_sem, c, replica)

    keep_sum = pltpu.make_async_copy(own_ref.at[0, : r_ref.shape[0], :], r_ref, out_sem)

    def dx_out(start, rows, k):
        sl = pl.ds(pl.multiple_of(start, 16), rows)
        return pltpu.make_async_copy(acc_ref.at[sl, :], dxp_ref.at[sl, :], dx_sem.at[k])

    third = TILE1 // 3
    dx_outs = [dx_out(t * TILE1, TILE1, t) for t in range(acc_ref.shape[0] // TILE1 - 1)]
    dx_lasts = [dx_out(acc_ref.shape[0] - TILE1 + k * third, third, len(dx_outs) + k) for k in range(3)]
    dw_outs = [pltpu.make_async_copy(dw_ref.at[k % 2], dws_ref.at[k], dw_sem.at[k]) for k in range(SHARDS1)]

    def take(s):
        def rows13(sl):
            w13_ref[sl, :] = w13s_ref[s, sl, :]

        def rows2(sl):
            w2c_ref[sl, :] = w2s_ref[s, sl, :]

        by_rows(w13_ref.shape[0], 128, rows13)
        by_rows(ff, 128, rows2)

    turns = (0, 1, SPREAD, tiles, FORWARD, 2 * tiles, ROW_SUM + CHUNKS)

    @seldom(functools.reduce(jnp.logical_or, [step == t for t in turns]))
    def _(_):
        barrier = pltpu.get_barrier_semaphore()

        @pl.when(step == 0)
        def _():
            for to in (mate, across, replica):
                pl.semaphore_signal(barrier, inc=1, device_id=to, device_id_type=MESH)

            def join(sl):
                w13_ref[sl, :ff] = w1_ref[sl, :]
                w13_ref[sl, ff:] = w3_ref[sl, :]

            def keep(sl):
                w2c_ref[sl, :] = w2_ref[sl, :]

            by_rows(w13_ref.shape[0], 128, join)
            by_rows(ff, 128, keep)

        @pl.when(step == 1)
        def _():
            pl.semaphore_wait(barrier, 3)
            for copy in (*to_row, *to_mate):
                copy.start()

        @pl.when(step == tiles)
        def _():
            for copy in to_mate:
                copy.wait_recv()
            take(0)
            dw_outs[0].start()

        @pl.when(step == 2 * tiles)
        def _():
            take(1)
            dw_outs[1].start()
            dw_outs[0].wait()

        @pl.when(step == SPREAD)
        def _():
            for copy in to_row:
                copy.wait_recv()
            for copy in spread:
                copy.start()

        @pl.when(step == FORWARD)
        def _():
            for copy in spread:
                copy.wait_recv()
            for copy in forward:
                copy.start()

        @pl.when(step == ROW_SUM + CHUNKS)
        def _():
            keep_sum.start()

    def chunk_at(lag):
        c = step - lag
        return jnp.where((c >= 0) & (c < CHUNKS), c, CHUNKS)

    def has_chunk(lag):
        return (step >= lag) & (step < lag + CHUNKS)

    @pl.when(has_chunk(1))
    def _():
        core_push(step - 1).start()

    @pl.when(has_chunk(2))
    def _():
        core_push(step - 2).wait_send()

    @pl.when(has_chunk(CORE_SUM + 1))
    def _():
        row_push(step - CORE_SUM - 1).start()

    @pl.when(has_chunk(CORE_SUM))
    def _():
        core_push(step - CORE_SUM).wait_recv()

    @pl.when(has_chunk(ROW_SUM + 1))
    def _():
        dp_push(step - ROW_SUM - 1).start()

    @pl.when(has_chunk(ROW_SUM))
    def _():
        row_push(step - ROW_SUM).wait_recv()

    def reduce_chunks():
        now, summed, done = rows_of(chunk_at(0)), rows_of(chunk_at(CORE_SUM)), rows_of(chunk_at(ROW_SUM))
        own_ref[0, done, :] = own_ref[0, done, :] + row_ref[done, :]
        own_ref[:, summed, :] = own_ref[:, summed, :] + core_ref[:, summed, :]
        for k, r in enumerate((row, 1 - row)):
            mine = pl.ds(pl.multiple_of((2 * r + core) * ff, ff), ff)
            theirs = pl.ds(pl.multiple_of((2 * r + 1 - core) * ff, ff), ff)
            own_ref[k, now, :] = g_ref[:, mine].astype(jnp.bfloat16)
            send_ref[lax.rem(step, 2), k] = g_ref[:, theirs].astype(jnp.bfloat16)

    @pl.when(step > steps - tiles)
    def _():
        dx_out((tile - 1) * TILE1, TILE1, tile - 1).start()

    def put_dx(start, rows, dx):
        sl = pl.ds(pl.multiple_of(tile * TILE1 + start, 16), rows)
        acc_ref[sl, :] = jnp.where(shard == 0, 0.0, acc_ref[sl, :]) + dx

    def compute(**extra):
        backward_tile(x_ref, dy_ref, w13_ref, w2c_ref, z_ref, h_ref, dw_ref.at[lax.rem(shard, 2)], tile == 0, put_dx, reduce_chunks, **extra)

    @pl.when(step < steps - 1)
    def _():
        compute()

    @seldom(step == steps - 1)
    def _(_):
        compute(before=(None, dw_outs[2].start, dx_lasts[0].start))
        for copy in dx_lasts[1:]:
            copy.start()
        for copy in (*to_mate, *to_row, *spread):
            copy.wait_send()
        for copy in forward:
            copy.wait()
        for c in range(CHUNKS):
            row_push(c).wait_send()
            dp_push(c).wait()
        keep_sum.wait()
        for copy in (*dw_outs[1:], *dx_outs, *dx_lasts):
            copy.wait()


def run_first(x, dy, weights, g):
    tokens, d = x.shape
    ff = weights[0].shape[1]
    g_rows, g_cols = g.shape
    chunk = g_rows // CHUNKS
    tiles = tokens // TILE1
    hbm = pl.BlockSpec(memory_space=pltpu.HBM)
    tok = pl.BlockSpec((TILE1, d), lambda s, j: (j, 0))
    whole = lambda w: pl.BlockSpec(w.shape, lambda s, j: (0, 0), pipeline_mode=pl.Buffered(1))
    bf16, f32, dma = jnp.bfloat16, jnp.float32, pltpu.SemaphoreType.DMA
    return pl.pallas_call(
        first_kernel,
        grid=(SHARDS1, tiles),
        in_specs=[tok, tok, pl.BlockSpec((chunk, g_cols), lambda s, j: (jnp.minimum(s * tiles + j, CHUNKS - 1), 0)), *[whole(w) for w in weights]],
        out_specs=[hbm] * 6,
        out_shape=[
            jax.ShapeDtypeStruct((tokens, d), f32),
            jax.ShapeDtypeStruct((SHARDS1, 3, d, ff), f32),
            jax.ShapeDtypeStruct((d, 2 * ff), bf16),
            jax.ShapeDtypeStruct((ff, d), bf16),
            jax.ShapeDtypeStruct((g_rows, ff), bf16),
            jax.ShapeDtypeStruct((g_rows, ff), bf16),
        ],
        scratch_shapes=[
            pltpu.VMEM((tokens, d), f32),
            pltpu.VMEM((2, 3, d, ff), f32),
            pltpu.VMEM((d, 2 * ff), bf16),
            pltpu.VMEM((ff, d), bf16),
            pltpu.VMEM((SHARDS1 - 1, d, 2 * ff), bf16),
            pltpu.VMEM((SHARDS1 - 1, ff, d), bf16),
            pltpu.VMEM((TILE1, 2 * ff), bf16),
            pltpu.VMEM((TILE1, ff), bf16),
            pltpu.VMEM((2, 2, chunk, ff), bf16),
            pltpu.VMEM((2, g_rows + chunk, ff), bf16),
            pltpu.VMEM((2, g_rows + chunk, ff), bf16),
            pltpu.VMEM((g_rows + chunk, ff), bf16),
            dma((2, 3)),
            dma((2, 3)),
            dma((2, 3)),
            dma((2, 3)),
            dma((2, CHUNKS)),
            dma((2, CHUNKS)),
            dma((2, CHUNKS)),
            dma(()),
            dma((tiles + 2,)),
            dma((SHARDS1,)),
        ],
        compiler_params=pltpu.CompilerParams(
            vmem_limit_bytes=VMEM_BYTES, dimension_semantics=("arbitrary", "arbitrary"), collective_id=0, has_side_effects=True
        ),
        cost_estimate=pl.CostEstimate(flops=16 * SHARDS1 * tokens * d * ff, bytes_accessed=120_000_000, transcendentals=0),
        name="bwd_first",
    )(x, dy, g, *weights)


def last_kernel(
    x_ref, dy_ref, w13_ref, w2_ref, r_ref, c_ref, dxp_ref, dws_ref,
    dx_ref, next_ref, dw_ref,
    z_ref, h_ref, dw_acc, move_ref, in_sem, move_sem, own_sem,
):
    tile, tiles = pl.program_id(0), pl.num_programs(0)
    row, core = lax.axis_index("row"), lax.axis_index("fsdp")
    ff = h_ref.shape[1]

    cols = [2 * row + core, 2 * row + 1 - core, 2 * (1 - row) + core, 2 * (1 - row) + 1 - core]
    lanes = [pl.ds(pl.multiple_of(q * ff, ff), ff) for q in cols]
    moves = dws_ref.shape[2] // MOVE

    def span(m):
        return pl.ds(pl.multiple_of(m * MOVE, MOVE), MOVE)

    def fetch(m):
        return pltpu.make_async_copy(dws_ref.at[:, :, span(m), :], move_ref.at[lax.rem(m, 2)], in_sem.at[lax.rem(m, 2)])

    def place(m):
        return [pltpu.make_async_copy(move_ref.at[lax.rem(m, 2), s], dw_ref.at[:, span(m), lanes[s]], move_sem.at[lax.rem(m, 2), s]) for s in range(SHARDS1)]

    @pl.when((tile >= 2) & (tile < moves + 2))
    def _():
        for copy in place(tile - 2):
            copy.wait()

    @pl.when(tile < moves)
    def _():
        fetch(tile).start()

    @pl.when((tile >= 1) & (tile < moves + 1))
    def _():
        fetch(tile - 1).wait()
        for copy in place(tile - 1):
            copy.start()

    def put_dx(start, rows, dx):
        sl = pl.ds(start, rows)
        dx_ref[sl, :] = (dxp_ref[sl, :] + dx).astype(jnp.bfloat16)

    def add_replicas():
        next_ref[...] = r_ref[...].astype(jnp.float32) + c_ref[...].astype(jnp.float32)

    def compute(**extra):
        backward_tile(x_ref, dy_ref, w13_ref, w2_ref, z_ref, h_ref, dw_acc, tile == 0, put_dx, add_replicas, **extra)

    @pl.when(tile < tiles - 1)
    def _():
        compute()

    @pl.when(tile == tiles - 1)
    def _():
        own = pltpu.make_async_copy(dw_acc, dw_ref.at[:, :, lanes[3]], own_sem)
        compute(before=(None, own.start))
        own.wait()


def run_last(x, dy, dxp, dws, weights, mine, other):
    tokens, d = x.shape
    ff = weights[1].shape[0]
    tiles = tokens // TILE2
    hbm = pl.BlockSpec(memory_space=pltpu.HBM)
    g_rows = mine.shape[0]
    tok = pl.BlockSpec((TILE2, d), lambda j: (j, 0))
    full = lambda w: pl.BlockSpec(w.shape, lambda j: (0, 0))
    part = pl.BlockSpec((g_rows // tiles, ff), lambda j: (j, 0))
    return pl.pallas_call(
        last_kernel,
        grid=(tiles,),
        in_specs=[tok, tok, *[full(w) for w in weights], part, part, tok, hbm],
        out_specs=[tok, part, hbm],
        out_shape=[
            jax.ShapeDtypeStruct((tokens, d), jnp.bfloat16),
            jax.ShapeDtypeStruct((g_rows, ff), jnp.float32),
            jax.ShapeDtypeStruct((3, d, 4 * ff), jnp.float32),
        ],
        scratch_shapes=[
            pltpu.VMEM((TILE2, 2 * ff), jnp.bfloat16),
            pltpu.VMEM((TILE2, ff), jnp.bfloat16),
            pltpu.VMEM((3, d, ff), jnp.float32),
            pltpu.VMEM((2, SHARDS1, 3, MOVE, ff), jnp.float32),
            pltpu.SemaphoreType.DMA((2,)),
            pltpu.SemaphoreType.DMA((2, SHARDS1)),
            pltpu.SemaphoreType.DMA(()),
        ],
        compiler_params=pltpu.CompilerParams(vmem_limit_bytes=VMEM_BYTES, dimension_semantics=("arbitrary",)),
        cost_estimate=pl.CostEstimate(flops=16 * tokens * d * ff, bytes_accessed=90_000_000, transcendentals=0),
        name="bwd_last",
    )(x, dy, *weights, mine, other, dxp, dws)


def solution(mesh):
    def local_step(x_dev, dy_dev, gate_shard, up_shard, down_shard, g_dev):
        micro_count, tok_dev, d_model = x_dev.shape
        ff = gate_shard.shape[1]
        x, dy = (v.reshape(micro_count * tok_dev, d_model) for v in (x_dev, dy_dev))
        g = g_dev.reshape(3 * d_model, 4 * ff)
        dxp, dws, *far, mine, other = run_first(x, dy, (gate_shard, up_shard, down_shard), g)
        dx, grad_next, grad_layer = run_last(x, dy, dxp, dws, far, mine, other)
        return dx.reshape(micro_count, tok_dev, d_model), grad_next.reshape(3, d_model, ff), grad_layer[None]

    in_specs = (P(None, TOK_AXES, None), P(None, TOK_AXES, None), P(None, GROUP_AXES), P(None, GROUP_AXES), P(GROUP_AXES, None), P(TOK_AXES, None, None, None))
    out_specs = (P(None, TOK_AXES, None), P(None, None, GROUP_AXES), P(TOK_AXES, None, None, None))
    return jax.shard_map(local_step, mesh=mesh, in_specs=in_specs, out_specs=out_specs, check_vma=False)
```
